512 devices in a mesh: gy: 8 (over x, core), gx: 64 (over z, y).
Axes of the slice: x: 4, y: 8, z: 8, core: 2. Of those that a mesh axis runs over, the one named last changes fastest.
Arguments:
- position: float32 [16, 512, 128, 3], P('gy', 'gx'), may hold values from 0 to 1
- velocity: float32 [16, 512, 128, 3], P('gy', 'gx'), may hold values from -6 to 6
- particle_mass: float32 [16, 512, 128], P('gy', 'gx'), may hold values from 0.006 to 0.025
- cell_counts: int32 [16, 512], P('gy', 'gx'), may hold values from 64 to 128
- shear_shift: int32 [1], replicated, may hold values from 252 to 260
Outputs:
- density: float32 [16, 512, 128], P('gy', 'gx')
- acceleration: float32 [16, 512, 128, 3], P('gy', 'gx')
The draws below stay inside these ranges and needn't reach their ends.
Inputs may be any that keep to these rules, and one draw needn't show every extreme that they name: `shear_shift`: the offset is a whole number of cells from 252 to 260.
All inputs are finite; a program needn't handle non-finite values.
Results may differ from the reference program's by a relative error of at most 0.0003.
Values sent between devices are 32-bit elements; how exact they have to be, the bound alone decides.
A program may use at most 64 MiB of HBM per device.

```python
import math
import jax
import jax.numpy as jnp
from jax import lax

SLOTS = 128
CXD = 8
NXC = 512
NYC = 16


def set_ends(result, rng, least, top_value):
    place = [jax.random.randint(jax.random.fold_in(rng, axis), (), 0, length) for axis, length in enumerate(result.shape)]
    widest = result.shape.index(max(result.shape))
    beside = place[:widest] + [(place[widest] + 1) % result.shape[widest]] + place[widest + 1:]
    return result.at[tuple(place)].set(least).at[tuple(beside)].set(top_value)


def block_levels(rng, shape, split, low, largest):
    def one(axis_at, shards_of):
        heights = jax.random.uniform(jax.random.fold_in(jax.random.fold_in(rng, 6), axis_at), (shards_of,), jnp.float32, low / len(split), largest / len(split))
        return jnp.repeat(jnp.exp(heights), shape[axis_at] // shards_of).reshape((-1,) + (1,) * (len(shape) - axis_at - 1))

    level = one(*split[0])
    for cut in split[1:]:
        level = level * one(*cut)
    return level


def gaussian(rng, extent, width, reach, split=(), kind=jnp.bfloat16):
    entries = width * jax.random.normal(rng, extent, jnp.float32)
    if split:
        entries = entries * block_levels(rng, extent, split, -0.22, 0.18)
    return jnp.clip(entries, -reach, reach).astype(kind)


def setup_inputs(seed: int = 0) -> dict:
    streams_of = jax.random.split(jax.random.key(seed), 6)
    position = jnp.clip(1.0 * jax.random.uniform(streams_of[0], (NYC, NXC, SLOTS, 3), jnp.float32) ** block_levels(streams_of[0], (NYC, NXC, SLOTS, 3), ((0, 8), (1, 64)), -0.2, 0.2), 0.0, 1.0)
    velocity = gaussian(streams_of[1], (NYC, NXC, SLOTS, 3), 1.0, 6.0, ((0, 8), (1, 64)), jnp.float32)
    particle_mass = jnp.clip(jnp.exp(math.log(0.025) - 1.4271164 * jax.random.uniform(streams_of[2], (NYC, NXC, SLOTS), jnp.float32) ** block_levels(streams_of[2], (NYC, NXC, SLOTS), ((0, 8), (1, 64)), -0.2, 0.2)), 0.006, 0.025)
    cell_counts = set_ends(jax.random.randint(streams_of[3], (NYC, NXC), SLOTS // 2, SLOTS + 1), jax.random.fold_in(streams_of[3], 1), SLOTS // 2, SLOTS).astype(jnp.int32)
    shear_shift = jax.random.randint(streams_of[4], (1,), NXC // 2 - CXD // 2, NXC // 2 + CXD // 2 + 1).astype(jnp.int32)
    return dict(position=position, velocity=velocity, particle_mass=particle_mass, cell_counts=cell_counts, shear_shift=shear_shift)


SMOOTHING = 0.5
KERNEL_NORM = 1.0 / (math.pi * SMOOTHING ** 3)
SOUND_SQ = 0.2
VISCOSITY = 0.05
SOFTENING = 0.0025
SHEAR_JUMP = 1.0

def kernel_value(dist_sq):
    distance = jnp.sqrt(dist_sq)
    ratio = distance / SMOOTHING
    inner_part = 1.0 - 1.5 * ratio * ratio + 0.75 * ratio * ratio * ratio
    outer_part = 0.25 * jnp.maximum(2.0 - ratio, 0.0) ** 3
    return KERNEL_NORM * jnp.where(ratio < 1.0, inner_part, outer_part)

def kernel_slope(dist_sq):
    distance = jnp.sqrt(dist_sq)
    ratio = distance / SMOOTHING
    inner_part = (-3.0 + 2.25 * ratio) / (SMOOTHING * SMOOTHING)
    outer_part = -0.75 * jnp.maximum(2.0 - ratio, 0.0) ** 2 / (SMOOTHING * jnp.maximum(distance, SMOOTHING))
    return KERNEL_NORM * jnp.where(ratio < 1.0, inner_part, outer_part)

def stencil(padded, row_index):
    band = lax.dynamic_slice_in_dim(padded, row_index, 3, 0)
    columns = padded.shape[1] - 2
    cell_offsets = []
    for up_down in range(3):
        for across in range(3):
            shifted = band[up_down, across:across + columns]
            cell_offsets.append(shifted)
    return jnp.concatenate(cell_offsets, axis=1)

def stencil_offsets(slots, channels, dtype):
    parts = []
    for up_down in range(3):
        for across in range(3):
            entry = jnp.array([across - 1.0, up_down - 1.0, 0.0], dtype)
            parts.append(jnp.broadcast_to(entry, (slots, 3)))
    return jnp.concatenate(parts, axis=0)

def own_cells(padded, row_index):
    return lax.dynamic_slice_in_dim(padded, row_index + 1, 1, 0)[0, 1:-1]

def pair_offsets(own_part, near_cells):
    shift_table = stencil_offsets(own_part.shape[1], near_cells.shape[-1], near_cells.dtype)
    near_pos = near_cells[:, :, 0:3] + shift_table[None]
    return own_part[:, :, None, 0:3] - near_pos[:, None, :, :]

def densities(padded):

    def one_row(row_index):
        near_cells = stencil(padded, row_index)
        own_part = own_cells(padded, row_index)
        offsets = pair_offsets(own_part, near_cells)
        dist_sq = lax.optimization_barrier(jnp.sum(offsets * offsets, axis=-1))
        return lax.optimization_barrier(jnp.sum(near_cells[:, None, :, 6] * kernel_value(dist_sq), axis=-1))
    return lax.map(one_row, jnp.arange(padded.shape[0] - 2, dtype=jnp.int32))

def forces(padded, rho_pad):
    rho_cells = rho_pad[..., None]

    def one_row(row_index):
        near_cells = stencil(padded, row_index)
        near_rho = stencil(rho_cells, row_index)[:, None, :, 0]
        own_part = own_cells(padded, row_index)
        own_rho = own_cells(rho_cells, row_index)
        offsets = pair_offsets(own_part, near_cells)
        dist_sq = lax.optimization_barrier(jnp.sum(offsets * offsets, axis=-1))
        slope = kernel_slope(dist_sq)
        near_mass = near_cells[:, None, :, 6]
        pressure_term = -(SOUND_SQ / own_rho + SOUND_SQ / near_rho) * near_mass * slope
        viscous_term = 2.0 * VISCOSITY * near_mass * slope * dist_sq / ((dist_sq + SOFTENING) * own_rho * near_rho)
        relative = own_part[:, :, None, 3:6] - near_cells[:, None, :, 3:6]
        return lax.optimization_barrier(jnp.sum(pressure_term[..., None] * offsets + viscous_term[..., None] * relative, axis=2))
    return lax.map(one_row, jnp.arange(padded.shape[0] - 2, dtype=jnp.int32))

def pad_global(fields, shift_cells, vx_jump):
    upper_rows = jnp.roll(fields[0], shift_cells, axis=0) + vx_jump
    lower_rows = jnp.roll(fields[-1], -shift_cells, axis=0) - vx_jump
    padded_y = jnp.concatenate([lower_rows[None], fields, upper_rows[None]], axis=0)
    return jnp.concatenate([padded_y[:, -1:], padded_y, padded_y[:, :1]], axis=1)

def reference(position, velocity, particle_mass, cell_counts, shear_shift):
    shift_cells = shear_shift[0]
    slots = position.shape[2]
    is_valid = jnp.arange(slots, dtype=jnp.int32)[None, None, :] < cell_counts[:, :, None]
    weight = jnp.where(is_valid, particle_mass, 0.0)
    fields = jnp.concatenate([position, velocity, weight[..., None]], axis=-1)
    vx_jump = jnp.array([0.0, 0.0, 0.0, SHEAR_JUMP, 0.0, 0.0, 0.0], fields.dtype)
    padded = pad_global(fields, shift_cells, vx_jump)
    density_raw = densities(padded)
    safe_rho = jnp.where(is_valid, density_raw, 1.0)
    rho_pad = pad_global(safe_rho[..., None], shift_cells, jnp.zeros((1,), fields.dtype))[..., 0]
    accel = forces(padded, rho_pad)
    density = jnp.where(is_valid, density_raw, 0.0)
    acceleration = jnp.where(is_valid[..., None], accel, 0.0)
    return (density, acceleration)
```

```python
import functools
import math

import jax
import jax.numpy as jnp
from jax import lax
from jax.experimental import pallas as pl
from jax.experimental.pallas import tpu as pltpu
from jax.sharding import PartitionSpec as P

SMOOTHING = 0.5
KERNEL_NORM = 1.0 / (math.pi * SMOOTHING**3)
SOUND_SQ = 0.2
VISCOSITY = 0.05
SOFTENING = 0.0025
SHEAR_JUMP = 1.0

MESH = pl.DeviceIdType.MESH
F32 = jnp.float32
BF16 = jnp.bfloat16
RHO_SCALE = KERNEL_NORM * 0.25
GRAD_SCALE = KERNEL_NORM * 0.75 / (SMOOTHING * SMOOTHING)
SOFT_Q = SOFTENING / (SMOOTHING * SMOOTHING)
TINY_Q = 1e-8
SLOTS = 128
ROWS = 2
COLS = 8
EDGE = 5
WINDOW = 2 * EDGE + COLS


def pieces(p):
    high = p.astype(BF16).astype(F32)
    rest = p - high
    middle = rest.astype(BF16).astype(F32)
    return high, middle, rest - middle


def zeros(n):
    return jnp.zeros((n, SLOTS), F32)


def kernel(
    ny, nx,
    counts, shift, pos, vel, mass,
    dens_out, acc_out,
    own_a, own_v, own_m,
    below_a, below_v, below_m,
    above_a, above_v, above_m,
    side_a, side_v, side_m,
    near, centre, feats, mass_cols,
    g_high, g_low, e_part,
    rho_part, sums,
    send_sem, recv_sem,
):
    gy, gx = lax.axis_index("gy"), lax.axis_index("gx")
    top = gy // (ny - 1)
    bottom = (ny - 1 - gy) // (ny - 1)
    half = nx // 2
    up_y, down_y = lax.rem(gy + 1, ny), lax.rem(gy + ny - 1, ny)

    def up_id(k):
        return (up_y, lax.rem(gx + half * top + k + nx, nx))

    def down_id(k):
        return (down_y, lax.rem(gx + half * bottom + k + nx, nx))

    left_id = (gy, lax.rem(gx + nx - 1, nx))
    right_id = (gy, lax.rem(gx + 1, nx))

    row_a, row_v, row_m = (below_a, above_a), (below_v, above_v), (below_m, above_m)
    barrier = pltpu.get_barrier_semaphore()
    for k in (0, -1, 1):
        pl.semaphore_signal(barrier, inc=1, device_id=up_id(k), device_id_type=MESH)
        pl.semaphore_signal(barrier, inc=1, device_id=down_id(k), device_id_type=MESH)
    pl.semaphore_signal(barrier, inc=1, device_id=left_id, device_id_type=MESH)
    pl.semaphore_signal(barrier, inc=1, device_id=right_id, device_id_type=MESH)

    def copy_of(phase, slot, src, dst, device):
        return pltpu.make_async_remote_copy(
            src_ref=src,
            dst_ref=dst,
            send_sem=send_sem.at[phase, slot],
            recv_sem=recv_sem.at[phase, slot],
            device_id=device,
            device_id_type=MESH,
        )

    spans = {
        1: (COLS - EDGE, EDGE, 0),
        0: (0, COLS, EDGE),
        -1: (0, EDGE, EDGE + COLS),
    }

    def copies(phase, own, row, side):
        out = []
        for k in (0, -1, 1):
            start, count, at = spans[k]
            out.append(copy_of(phase, 1 - k, own.at[1, pl.ds(start, count)], row[0].at[pl.ds(at, count)], up_id(k)))
            out.append(copy_of(phase, 4 - k, own.at[0, pl.ds(start, count)], row[1].at[pl.ds(at, count)], down_id(k)))
        out.append(copy_of(phase, 6, own.at[:, COLS - 1], side.at[0], right_id))
        out.append(copy_of(phase, 7, own.at[:, 0], side.at[1], left_id))
        return out

    def wait_row(phase, own, row, d):
        for k in (0, -1, 1):
            start, count, at = spans[k]
            copy_of(phase, 3 * d + 1 - k, own.at[0, pl.ds(start, count)], row[d].at[pl.ds(at, count)], left_id).wait_recv()

    def wait_side(phase, own, side):
        for s in (0, 1):
            copy_of(phase, 6 + s, own.at[:, 0], side.at[s], left_id).wait_recv()

    lane = lax.broadcasted_iota(jnp.int32, (COLS, SLOTS), 1)
    column = lax.broadcasted_iota(jnp.int32, (COLS, SLOTS), 0).astype(F32)

    def valid_of(r):
        bound = jnp.concatenate([jnp.full((1, SLOTS), counts[r, c], jnp.int32) for c in range(COLS)], axis=0)
        return lane < bound

    for r in range(ROWS):
        fields = [pos[r, 0], pos[r, 1], pos[r, 2], jnp.where(valid_of(r), mass[r], 0.0)]
        for f in range(4):
            for c in range(COLS):
                own_a[r, c, f : f + 1, :] = fields[f][c : c + 1, :]
        for f in range(3):
            for c in range(COLS):
                own_v[r, c, f : f + 1, :] = vel[r, f][c : c + 1, :]
        for c in range(COLS):
            own_v[r, c, 3:4, :] = zeros(1)

    def prepare(e, j, xyzw):
        e_f = e.astype(F32) if hasattr(e, "astype") else float(e)
        x = 2.0 * xyzw[0:1] + (2.0 * j - 10.0)
        y = 2.0 * xyzw[1:2] + (2.0 * e_f - 4.0)
        z = 2.0 * xyzw[2:3] - 1.0
        w = xyzw[3:4]
        n = x * x + y * y + z * z
        one = jnp.ones((1, SLOTS), F32)
        lhs = jnp.concatenate([x, y, z, n, one, w, zeros(2)], axis=0)
        high, middle, low = pieces(lhs)
        table = jnp.concatenate([high, high, high, middle, middle, low, lhs, zeros(8)], axis=0).T
        near[e, j * SLOTS : (j + 1) * SLOTS, :] = table.astype(BF16)
        mass_cols[e, j * SLOTS : (j + 1) * SLOTS, :] = jnp.broadcast_to(table[:, 53:54], (SLOTS, SLOTS))
        first = jnp.concatenate([w, w * x, w * y, w * z, zeros(4)], axis=0)
        feats[e, 32:64, j * SLOTS : (j + 1) * SLOTS] = jnp.concatenate([*pieces(first), zeros(8)], axis=0).astype(BF16)
        return x, y, z, n, one

    def prepare_own(r, carry):
        for c in range(COLS):
            x, y, z, n, one = prepare(r + 1, c + 1, own_a[r, c])
            rhs = jnp.concatenate([-2.0 * x, -2.0 * y, -2.0 * z, one, n, zeros(3)], axis=0)
            high, middle, low = pieces(rhs)
            centre[r, c] = jnp.concatenate([high, middle, low, high, middle, high, zeros(16)], axis=0).astype(BF16)
        return carry

    lax.fori_loop(0, ROWS, prepare_own, 0)
    rho_part[...] = jnp.zeros_like(rho_part)
    sums[...] = jnp.zeros_like(sums)

    pl.semaphore_wait(barrier, 8)
    sent = copies(0, own_a, row_a, side_a) + copies(1, own_v, row_v, side_v)
    for copy in sent:
        copy.start()

    def pairs(r, a, c):
        e = r + a
        total = rho_part[r, c]
        rhs = centre[r, c]
        for b in range(3):
            at = (c + b) * SLOTS
            q_sq = jnp.dot(near[e, at : at + SLOTS, :], rhs, preferred_element_type=F32)
            q_sq = jnp.maximum(q_sq, TINY_Q)
            inverse = lax.rsqrt(q_sq)
            q = q_sq * inverse
            u = jnp.maximum(2.0 - q, 0.0)
            s = jnp.maximum(1.0 - q, 0.0)
            u_sq = u * u
            s_sq = 4.0 * (s * s)
            value = u_sq * u - s_sq * s
            slope = (s_sq - u_sq) * inverse
            soft = lax.rsqrt(q_sq + SOFT_Q)
            extra = (slope * soft) * soft
            weighted = value * mass_cols[e, at : at + SLOTS, :]
            total = total + jnp.sum(weighted.reshape(SLOTS // 8, 8, SLOTS), axis=0)
            high = slope.astype(BF16)
            span = pl.ds(b * SLOTS, SLOTS)
            g_high[r, a, c, span, :] = high
            g_low[r, a, c, span, :] = (slope - high.astype(F32)).astype(BF16)
            e_part[r, a, c, span, :] = extra.astype(BF16)
        rho_part[r, c] = total

    def reduce(r, a, c):
        e = r + a
        lanes = pl.ds(c * SLOTS, 3 * SLOTS)
        rows = feats[e, :, lanes]
        g = jnp.dot(rows, g_high[r, a, c], preferred_element_type=F32)
        g = g + jnp.dot(rows, g_low[r, a, c], preferred_element_type=F32)
        v = jnp.dot(rows[0:32], e_part[r, a, c], preferred_element_type=F32)
        sums[r, c, 0:8, :] += g[0:8] + g[8:16] + g[16:24]
        sums[r, c, 8:16, :] += g[32:40] + g[40:48] + g[48:56]
        sums[r, c, 16:24, :] += v[0:8] + v[8:16] + v[16:24]

    def own_units(work, cells):
        def body(t, carry):
            r = t // 2
            a = 1 - r + lax.rem(t, 2)
            for c in cells:
                work(r, a, c)
            return carry

        lax.fori_loop(0, 4, body, 0)

    inner, outer = tuple(range(1, COLS - 1)), (0, COLS - 1)
    own_units(pairs, inner)
    wait_side(0, own_a, side_a)
    for s in (0, 1):
        for r in range(ROWS):
            prepare(r + 1, (COLS + 1) * s, side_a[s, r])
    own_units(pairs, outer)

    s_cells = shift[0]
    base = EDGE - 1
    drift = jnp.clip(s_cells - half * COLS, -base, base)

    starts = (base + bottom * drift, base - top * drift)

    def both_rows(work):
        pl.when(bottom == 1)(lambda: work(1))
        work(0)
        pl.when(bottom == 0)(lambda: work(1))

    def ghost_pairs(d):
        wait_row(0, own_a, row_a, d)
        for j in range(COLS + 2):
            prepare(3 * d, j, row_a[d][starts[d] + j])
        for c in range(COLS):
            pairs(d, 2 * d, c)

    both_rows(ghost_pairs)

    valid = [valid_of(r) for r in range(ROWS)]
    inverse_rho = []
    for r in range(ROWS):
        rho = jnp.concatenate([jnp.sum(rho_part[r, c], axis=0, keepdims=True) for c in range(COLS)], axis=0) * RHO_SCALE
        dens_out[r] = jnp.where(valid[r], rho, 0.0)
        inv = 1.0 / jnp.where(valid[r], rho, 1.0)
        inverse_rho.append(inv)
        ratio = jnp.where(valid[r], mass[r], 0.0) * inv
        for c in range(COLS):
            own_m[r, c] = ratio[c : c + 1, :]
    sent_m = copies(2, own_m, row_m, side_m)
    for copy in sent_m:
        copy.start()

    def second(e, j, xyzw, v, ratio, jump):
        e_f = e.astype(F32) if hasattr(e, "astype") else float(e)
        x = 2.0 * xyzw[0:1] + (2.0 * j - 10.0)
        y = 2.0 * xyzw[1:2] + (2.0 * e_f - 4.0)
        z = 2.0 * xyzw[2:3] - 1.0
        block = jnp.concatenate(
            [ratio, ratio * x, ratio * y, ratio * z, ratio * (v[0:1] + jump), ratio * v[1:2], ratio * v[2:3], zeros(1)],
            axis=0,
        )
        feats[e, 0:32, j * SLOTS : (j + 1) * SLOTS] = jnp.concatenate([*pieces(block), zeros(8)], axis=0).astype(BF16)

    def second_own(r, carry):
        for c in range(COLS):
            second(r + 1, c + 1, own_a[r, c], own_v[r, c], own_m[r, c], 0.0)
        return carry

    lax.fori_loop(0, ROWS, second_own, 0)
    own_units(reduce, inner)
    wait_side(1, own_v, side_v)
    wait_side(2, own_m, side_m)
    for s in (0, 1):
        for r in range(ROWS):
            second(r + 1, (COLS + 1) * s, side_a[s, r], side_v[s, r], side_m[s, r], 0.0)
    own_units(reduce, outer)

    jumps = (-(bottom.astype(F32)) * SHEAR_JUMP, top.astype(F32) * SHEAR_JUMP)

    def ghost_reduce(d):
        wait_row(1, own_v, row_v, d)
        wait_row(2, own_m, row_m, d)
        for j in range(COLS + 2):
            at = starts[d] + j
            second(3 * d, j, row_a[d][at], row_v[d][at], row_m[d][at], jumps[d])
        for c in range(COLS):
            reduce(d, 2 * d, c)

    both_rows(ghost_reduce)

    for r in range(ROWS):
        def row_of(k):
            return jnp.concatenate([sums[r, c, k : k + 1, :] for c in range(COLS)], axis=0)

        scaled = [
            2.0 * pos[r, 0] + (2.0 * column - 8.0),
            2.0 * pos[r, 1] + (2.0 * r - 2.0),
            2.0 * pos[r, 2] - 1.0,
        ]
        inv = inverse_rho[r]
        ratio_sum, mass_sum = row_of(0), row_of(8)
        visc_sum = ratio_sum - SOFT_Q * row_of(16)
        for f in range(3):
            far = scaled[f] * ratio_sum - row_of(1 + f)
            near_part = scaled[f] * mass_sum - row_of(9 + f)
            drag = vel[r, f] * visc_sum - (row_of(4 + f) - SOFT_Q * row_of(20 + f))
            total = (-0.5 * SOUND_SQ * GRAD_SCALE) * (inv * near_part + far) + (2.0 * VISCOSITY * GRAD_SCALE) * (inv * drag)
            acc_out[r, f] = jnp.where(valid[r], total, 0.0)

    for copy in sent + sent_m:
        copy.wait_send()


def local(ny, nx, position, velocity, particle_mass, cell_counts, shear_shift):
    pos = jnp.transpose(position, (0, 3, 1, 2))
    vel = jnp.transpose(velocity, (0, 3, 1, 2))
    vmem = pl.BlockSpec(memory_space=pltpu.VMEM)
    smem = pl.BlockSpec(memory_space=pltpu.SMEM)
    table = (ROWS, 3, COLS, 3 * SLOTS, SLOTS)
    density, accel = pl.pallas_call(
        functools.partial(kernel, ny, nx),
        out_shape=(
            jax.ShapeDtypeStruct((ROWS, COLS, SLOTS), F32),
            jax.ShapeDtypeStruct((ROWS, 3, COLS, SLOTS), F32),
        ),
        in_specs=[smem, smem, vmem, vmem, vmem],
        out_specs=(vmem, vmem),
        scratch_shapes=[
            pltpu.VMEM((ROWS, COLS, 4, SLOTS), F32),
            pltpu.VMEM((ROWS, COLS, 4, SLOTS), F32),
            pltpu.VMEM((ROWS, COLS, 1, SLOTS), F32),
            pltpu.VMEM((WINDOW, 4, SLOTS), F32),
            pltpu.VMEM((WINDOW, 4, SLOTS), F32),
            pltpu.VMEM((WINDOW, 1, SLOTS), F32),
            pltpu.VMEM((WINDOW, 4, SLOTS), F32),
            pltpu.VMEM((WINDOW, 4, SLOTS), F32),
            pltpu.VMEM((WINDOW, 1, SLOTS), F32),
            pltpu.VMEM((2, ROWS, 4, SLOTS), F32),
            pltpu.VMEM((2, ROWS, 4, SLOTS), F32),
            pltpu.VMEM((2, ROWS, 1, SLOTS), F32),
            pltpu.VMEM((ROWS + 2, (COLS + 2) * SLOTS, 64), BF16),
            pltpu.VMEM((ROWS, COLS, 64, SLOTS), BF16),
            pltpu.VMEM((ROWS + 2, 64, (COLS + 2) * SLOTS), BF16),
            pltpu.VMEM((ROWS + 2, (COLS + 2) * SLOTS, SLOTS), F32),
            pltpu.VMEM(table, BF16),
            pltpu.VMEM(table, BF16),
            pltpu.VMEM(table, BF16),
            pltpu.VMEM((ROWS, COLS, 8, SLOTS), F32),
            pltpu.VMEM((ROWS, COLS, 24, SLOTS), F32),
            pltpu.SemaphoreType.DMA((3, 8)),
            pltpu.SemaphoreType.DMA((3, 8)),
        ],
        compiler_params=pltpu.CompilerParams(
            collective_id=0, has_side_effects=True, vmem_limit_bytes=48 * 1024 * 1024
        ),
        name="sph_step",
    )(cell_counts, shear_shift, pos, vel, particle_mass)
    return density, jnp.transpose(accel, (0, 2, 3, 1))


def solution(mesh):
    placed = (
        P("gy", "gx", None, None),
        P("gy", "gx", None, None),
        P("gy", "gx", None),
        P("gy", "gx"),
        P(),
    )
    return jax.shard_map(
        functools.partial(local, mesh.shape["gy"], mesh.shape["gx"]),
        mesh=mesh,
        in_specs=placed,
        out_specs=(P("gy", "gx", None), P("gy", "gx", None, None)),
        check_vma=False,
    )
```

```python
import functools
import math

import jax
import jax.numpy as jnp
from jax import lax
from jax.experimental import pallas as pl
from jax.experimental.pallas import tpu as pltpu
from jax.sharding import PartitionSpec as P

SMOOTHING = 0.5
KERNEL_NORM = 1.0 / (math.pi * SMOOTHING**3)
SOUND_SQ = 0.2
VISCOSITY = 0.05
SOFTENING = 0.0025
SHEAR_JUMP = 1.0

MESH = pl.DeviceIdType.MESH
F32 = jnp.float32
BF16 = jnp.bfloat16
RHO_SCALE = KERNEL_NORM * 0.25
GRAD_SCALE = KERNEL_NORM * 0.75 / (SMOOTHING * SMOOTHING)
SOFT_Q = SOFTENING / (SMOOTHING * SMOOTHING)
TINY_Q = 1e-8
SLOTS = 128
ROWS = 2
COLS = 8
WIDTH = (2, 1, 1)
DRIFT = 4
EDGE = tuple(w + DRIFT for w in WIDTH)
WINDOW = tuple(2 * e + COLS for e in EDGE)
FAR = 3
EXTRA = 4


def pieces(p):
    high = p.astype(BF16).astype(F32)
    rest = p - high
    middle = rest.astype(BF16).astype(F32)
    return high, middle, rest - middle


def zeros(n):
    return jnp.zeros((n, SLOTS), F32)


def kernel(
    ny, nx,
    counts_in, shift, pos_in, vel_in, mass_in,
    dens_out, acc_out,
    own_a, own_v, own_m,
    below_a, below_v, below_m,
    above_a, above_v, above_m,
    side_a, side_v, side_m,
    far_a, far_m,
    near, centre, far_centre, feats, mass_cols,
    g_high, g_low, e_part,
    rho_part, sums,
    counts, pos, vel, mass,
    send_sem, recv_sem, load_sem,
):
    gy, gx = lax.axis_index("gy"), lax.axis_index("gx")
    top = gy // (ny - 1)
    bottom = (ny - 1 - gy) // (ny - 1)
    half = nx // 2
    up_y, down_y = lax.rem(gy + 1, ny), lax.rem(gy + ny - 1, ny)

    def up_id(k):
        return (up_y, lax.rem(gx + half * top + k + nx, nx))

    def down_id(k):
        return (down_y, lax.rem(gx + half * bottom + k + nx, nx))

    left_id = (gy, lax.rem(gx + nx - 1, nx))
    right_id = (gy, lax.rem(gx + 1, nx))

    row_a, row_v, row_m = (below_a, above_a), (below_v, above_v), (below_m, above_m)
    barrier = pltpu.get_barrier_semaphore()
    for k in (0, -1, 1):
        pl.semaphore_signal(barrier, inc=1, device_id=up_id(k), device_id_type=MESH)
        pl.semaphore_signal(barrier, inc=1, device_id=down_id(k), device_id_type=MESH)
    pl.semaphore_signal(barrier, inc=1, device_id=left_id, device_id_type=MESH)
    pl.semaphore_signal(barrier, inc=1, device_id=right_id, device_id_type=MESH)

    loads = [
        pltpu.make_async_copy(src, dst, load_sem.at[i])
        for i, (src, dst) in enumerate(
            ((counts_in, counts), (pos_in, pos), (mass_in, mass), (vel_in, vel))
        )
    ]
    for load in loads:
        load.start()

    def copy_of(phase, slot, src, dst, device):
        return pltpu.make_async_remote_copy(
            src_ref=src,
            dst_ref=dst,
            send_sem=send_sem.at[phase, slot],
            recv_sem=recv_sem.at[phase, slot],
            device_id=device,
            device_id_type=MESH,
        )

    def spans(edge):
        return ((1, COLS - edge, edge, 0), (0, 0, COLS, edge), (-1, 0, edge, edge + COLS))

    def row_copies(phase, slot, src, dst, device):
        return [
            copy_of(phase, slot - k, src.at[pl.ds(start, count)], dst.at[pl.ds(at, count)], device(k))
            for k, start, count, at in spans(EDGE[phase % FAR])
        ]

    def up_copies(phase, own, row):
        return row_copies(phase, 1, own.at[1], row[0], up_id)

    def down_copies(phase, own, row):
        return row_copies(phase, 4, own.at[0], row[1], down_id)

    def side_copies(phase, own, side):
        w = WIDTH[phase]
        return [
            copy_of(phase, 6, own.at[:, pl.ds(COLS - w, w)], side.at[0], right_id),
            copy_of(phase, 7, own.at[:, pl.ds(0, w)], side.at[1], left_id),
        ]

    def far_copies():
        return (
            row_copies(FAR, 1, own_a.at[0], far_a, up_id),
            row_copies(FAR, 1, own_a.at[1], far_a, down_id),
        )

    def start(copies):
        for copy in copies:
            copy.start()

    def wait_row(phase, own, row, d):
        for copy in row_copies(phase, 3 * d + 1, own.at[0], row[d], lambda k: left_id):
            copy.wait_recv()

    def wait_side(phase, own, side):
        for copy in side_copies(phase, own, side):
            copy.wait_recv()

    lane = lax.broadcasted_iota(jnp.int32, (COLS, SLOTS), 1)
    column = lax.broadcasted_iota(jnp.int32, (COLS, SLOTS), 0).astype(F32)

    def valid_of(r):
        bound = jnp.concatenate([jnp.full((1, SLOTS), counts[r, c], jnp.int32) for c in range(COLS)], axis=0)
        return lane < bound

    for load in loads:
        load.wait()
    for r in range(ROWS):
        fields = [pos[r, 0], pos[r, 1], pos[r, 2], jnp.where(valid_of(r), mass[r], 0.0)]
        for f in range(4):
            for c in range(COLS):
                own_a[r, c, f : f + 1, :] = fields[f][c : c + 1, :]
        for f in range(3):
            for c in range(COLS):
                own_v[r, c, f : f + 1, :] = vel[r, f][c : c + 1, :]
        for c in range(COLS):
            own_v[r, c, 3:4, :] = zeros(1)

    def scaled(xyzw, j, row):
        row = row.astype(F32) if hasattr(row, "astype") else float(row)
        x = 2.0 * xyzw[0:1] + (2.0 * j - 10.0)
        y = 2.0 * xyzw[1:2] + (2.0 * row - 4.0)
        return x, y, 2.0 * xyzw[2:3] - 1.0

    def prepare(e, j, xyzw, row=None):
        x, y, z = scaled(xyzw, j, e if row is None else row)
        w = xyzw[3:4]
        n = x * x + y * y + z * z
        lhs = jnp.concatenate([x, y, z, n, jnp.ones((1, SLOTS), F32), w, zeros(2)], axis=0)
        high, middle, low = pieces(lhs)
        table = jnp.concatenate([high, high, high, middle, middle, low, lhs, zeros(8)], axis=0).T
        at = (j + 1) * SLOTS
        near[e, at : at + SLOTS, :] = table.astype(BF16)
        mass_cols[e, at : at + SLOTS, :] = jnp.broadcast_to(table[:, 53:54], (SLOTS, SLOTS))
        if row is None and 0 <= j < COLS + 2:
            first = jnp.concatenate([w, w * x, w * y, w * z, zeros(4)], axis=0)
            feats[e, 32:64, j * SLOTS : (j + 1) * SLOTS] = jnp.concatenate([*pieces(first), zeros(8)], axis=0).astype(BF16)

    def centre_of(xyzw, j, row):
        x, y, z = scaled(xyzw, j, row)
        n = x * x + y * y + z * z
        rhs = jnp.concatenate([-2.0 * x, -2.0 * y, -2.0 * z, jnp.ones((1, SLOTS), F32), n, zeros(3)], axis=0)
        high, middle, low = pieces(rhs)
        return jnp.concatenate([high, middle, low, high, middle, high, zeros(16)], axis=0).astype(BF16)

    def prepare_own(r, carry):
        for c in range(COLS):
            prepare(r + 1, c + 1, own_a[r, c])
            centre[r, c] = centre_of(own_a[r, c], c + 1, r + 1)
        return carry

    lax.fori_loop(0, ROWS, prepare_own, 0)
    rho_part[...] = jnp.zeros_like(rho_part)
    sums[...] = jnp.zeros_like(sums)

    pl.semaphore_wait(barrier, 8)
    sent_a = up_copies(0, own_a, row_a) + down_copies(0, own_a, row_a) + side_copies(0, own_a, side_a)
    sent_v = up_copies(1, own_v, row_v) + down_copies(1, own_v, row_v) + side_copies(1, own_v, side_v)
    sent_up, sent_down = far_copies()
    start(sent_a)
    pl.when(top == 1)(lambda: start(sent_up))
    pl.when(bottom == 1)(lambda: start(sent_down))
    start(sent_v)

    def kernel_of(cells, rhs):
        q_sq = jnp.maximum(jnp.dot(cells, rhs, preferred_element_type=F32), TINY_Q)
        inverse = lax.rsqrt(q_sq)
        q = q_sq * inverse
        u = jnp.maximum(2.0 - q, 0.0)
        s = jnp.maximum(1.0 - q, 0.0)
        u_sq = u * u
        s_sq = 4.0 * (s * s)
        return u_sq * u - s_sq * s, (s_sq - u_sq) * inverse, q_sq

    def pairs(r, a, c):
        e = r + a
        total = rho_part[r, c]
        rhs = centre[r, c]
        for b in range(3):
            at = (c + b + 1) * SLOTS
            value, slope, q_sq = kernel_of(near[e, at : at + SLOTS, :], rhs)
            soft = lax.rsqrt(q_sq + SOFT_Q)
            extra = (slope * soft) * soft
            weighted = value * mass_cols[e, at : at + SLOTS, :]
            total = total + jnp.sum(weighted.reshape(SLOTS // 8, 8, SLOTS), axis=0)
            high = slope.astype(BF16)
            span = pl.ds(b * SLOTS, SLOTS)
            g_high[r, a, c, span, :] = high
            g_low[r, a, c, span, :] = (slope - high.astype(F32)).astype(BF16)
            e_part[r, a, c, span, :] = extra.astype(BF16)
        rho_part[r, c] = total

    def reduce(r, a, c):
        e = r + a
        lanes = pl.ds(c * SLOTS, 3 * SLOTS)
        rows = feats[e, :, lanes]
        g = jnp.dot(rows, g_high[r, a, c], preferred_element_type=F32)
        g = g + jnp.dot(rows, g_low[r, a, c], preferred_element_type=F32)
        v = jnp.dot(rows[0:32], e_part[r, a, c], preferred_element_type=F32)
        sums[r, c, 0:8, :] += g[0:8] + g[8:16] + g[16:24]
        sums[r, c, 8:16, :] += g[32:40] + g[40:48] + g[48:56]
        sums[r, c, 16:24, :] += v[0:8] + v[8:16] + v[16:24]

    def own_units(work, cells):
        def body(t, carry):
            r = t // 2
            a = 1 - r + lax.rem(t, 2)
            for c in cells:
                work(r, a, c)
            return carry

        lax.fori_loop(0, 4, body, 0)

    inner, outer = tuple(range(1, COLS - 1)), (0, COLS - 1)
    own_units(pairs, inner)
    wait_side(0, own_a, side_a)
    for s in (0, 1):
        for r in range(ROWS):
            prepare(r + 1, (COLS + 1) * s, side_a[s, r, 1 - s])
    own_units(pairs, outer)

    drift = jnp.clip(shift[0] - half * COLS, -DRIFT, DRIFT)
    drifts = (bottom * drift, -top * drift)
    far_side = (bottom, top)

    def window(phase, d, j):
        return EDGE[phase] - 1 + drifts[d] + j

    def both_rows(work):
        pl.when(bottom == 1)(lambda: work(1))
        work(0)
        pl.when(bottom == 0)(lambda: work(1))

    def ghost_pairs(d):
        wait_row(0, own_a, row_a, d)
        for j in range(COLS + 2):
            prepare(3 * d, j, row_a[d][window(0, d, j)])
        for c in range(COLS):
            pairs(d, 2 * d, c)

    both_rows(ghost_pairs)

    valid = [valid_of(r) for r in range(ROWS)]
    inverse_rho = []
    for r in range(ROWS):
        rho = jnp.concatenate([jnp.sum(rho_part[r, c], axis=0, keepdims=True) for c in range(COLS)], axis=0) * RHO_SCALE
        dens_out[r] = jnp.where(valid[r], rho, 0.0)
        inv = 1.0 / jnp.where(valid[r], rho, 1.0)
        inverse_rho.append(inv)
        ratio = jnp.where(valid[r], mass[r], 0.0) * inv
        for c in range(COLS):
            own_m[r, c] = ratio[c : c + 1, :]
    sent_m = up_copies(2, own_m, row_m), down_copies(2, own_m, row_m), side_copies(2, own_m, side_m)
    pl.when(top == 0)(lambda: start(sent_m[0]))
    pl.when(bottom == 0)(lambda: start(sent_m[1]))
    start(sent_m[2])

    def far_tables(d):
        for copy in row_copies(FAR, 1, own_a.at[0], far_a, lambda k: left_id):
            copy.wait_recv()
        for j in range(-1, COLS + 3):
            prepare(EXTRA, j, far_a[window(0, d, j)], row=5 * d - 1)
        for s in (0, 1):
            j = (COLS + 3) * s - 1
            prepare(3 * d, j, row_a[d][window(0, d, j)])
            prepare(d + 1, j, side_a[s, d, s])
        for j in range(COLS + 2):
            far_centre[j] = centre_of(row_a[d][window(0, d, j)], j, 3 * d)

    def far_density(d):
        def body(t, carry):
            for i in range(5):
                j = 5 * t + i
                total = zeros(8)
                rhs = far_centre[j]
                for e in (d + 1, 3 * d, EXTRA):
                    for b in range(3):
                        at = pl.multiple_of((j + b) * SLOTS, SLOTS)
                        value, _, _ = kernel_of(near[e, pl.ds(at, SLOTS), :], rhs)
                        weighted = value * mass_cols[e, pl.ds(at, SLOTS), :]
                        total = total + jnp.sum(weighted.reshape(SLOTS // 8, 8, SLOTS), axis=0)
                far_m[j] = jnp.sum(total, axis=0, keepdims=True) * RHO_SCALE
            return carry

        lax.fori_loop(0, 2, body, 0)

    pl.when(bottom == 1)(lambda: far_tables(0))
    pl.when(top == 1)(lambda: far_tables(1))
    pl.when(bottom + top == 1)(lambda: far_density(top))

    def second(e, j, xyzw, v, ratio, jump):
        x, y, z = scaled(xyzw, j, e)
        block = jnp.concatenate(
            [ratio, ratio * x, ratio * y, ratio * z, ratio * (v[0:1] + jump), ratio * v[1:2], ratio * v[2:3], zeros(1)],
            axis=0,
        )
        feats[e, 0:32, j * SLOTS : (j + 1) * SLOTS] = jnp.concatenate([*pieces(block), zeros(8)], axis=0).astype(BF16)

    def second_own(r, carry):
        for c in range(COLS):
            second(r + 1, c + 1, own_a[r, c], own_v[r, c], own_m[r, c], 0.0)
        return carry

    lax.fori_loop(0, ROWS, second_own, 0)
    own_units(reduce, inner)
    wait_side(1, own_v, side_v)
    wait_side(2, own_m, side_m)
    for s in (0, 1):
        for r in range(ROWS):
            second(r + 1, (COLS + 1) * s, side_a[s, r, 1 - s], side_v[s, r, 0], side_m[s, r, 0], 0.0)
    own_units(reduce, outer)

    jumps = (-(bottom.astype(F32)) * SHEAR_JUMP, top.astype(F32) * SHEAR_JUMP)

    def ghost_reduce(d):
        wait_row(1, own_v, row_v, d)
        pl.when(far_side[d] == 0)(lambda: wait_row(2, own_m, row_m, d))
        for j in range(COLS + 2):
            xyzw = row_a[d][window(0, d, j)]
            w = xyzw[3:4]
            far_ratio = w / jnp.where(w > 0.0, far_m[j], 1.0)
            ratio = jnp.where(far_side[d] == 1, far_ratio, row_m[d][window(2, d, j)])
            second(3 * d, j, xyzw, row_v[d][window(1, d, j)], ratio, jumps[d])
        for c in range(COLS):
            reduce(d, 2 * d, c)

    both_rows(ghost_reduce)

    for r in range(ROWS):
        def row_of(k):
            return jnp.concatenate([sums[r, c, k : k + 1, :] for c in range(COLS)], axis=0)

        block = [
            2.0 * pos[r, 0] + (2.0 * column - 8.0),
            2.0 * pos[r, 1] + (2.0 * r - 2.0),
            2.0 * pos[r, 2] - 1.0,
        ]
        inv = inverse_rho[r]
        ratio_sum, mass_sum = row_of(0), row_of(8)
        visc_sum = ratio_sum - SOFT_Q * row_of(16)
        for f in range(3):
            far = block[f] * ratio_sum - row_of(1 + f)
            near_part = block[f] * mass_sum - row_of(9 + f)
            drag = vel[r, f] * visc_sum - (row_of(4 + f) - SOFT_Q * row_of(20 + f))
            total = (-0.5 * SOUND_SQ * GRAD_SCALE) * (inv * near_part + far) + (2.0 * VISCOSITY * GRAD_SCALE) * (inv * drag)
            acc_out[r, f] = jnp.where(valid[r], total, 0.0)

    def drain(copies):
        for copy in copies:
            copy.wait_send()

    drain(sent_a + sent_v + sent_m[2])
    pl.when(top == 1)(lambda: drain(sent_up))
    pl.when(top == 0)(lambda: drain(sent_m[0]))
    pl.when(bottom == 1)(lambda: drain(sent_down))
    pl.when(bottom == 0)(lambda: drain(sent_m[1]))


def local(ny, nx, position, velocity, particle_mass, cell_counts, shear_shift):
    pos = jnp.transpose(position, (0, 3, 1, 2))
    vel = jnp.transpose(velocity, (0, 3, 1, 2))
    vmem = pl.BlockSpec(memory_space=pltpu.VMEM)
    hbm = pl.BlockSpec(memory_space=pltpu.HBM)
    in_hbm = functools.partial(pltpu.with_memory_space_constraint, memory_space=pltpu.HBM)
    table = (ROWS, 3, COLS, 3 * SLOTS, SLOTS)
    density, accel = pl.pallas_call(
        functools.partial(kernel, ny, nx),
        out_shape=(
            jax.ShapeDtypeStruct((ROWS, COLS, SLOTS), F32),
            jax.ShapeDtypeStruct((ROWS, 3, COLS, SLOTS), F32),
        ),
        in_specs=[hbm, pl.BlockSpec(memory_space=pltpu.SMEM), hbm, hbm, hbm],
        out_specs=(vmem, vmem),
        scratch_shapes=[
            pltpu.VMEM((ROWS, COLS, 4, SLOTS), F32),
            pltpu.VMEM((ROWS, COLS, 4, SLOTS), F32),
            pltpu.VMEM((ROWS, COLS, 1, SLOTS), F32),
            *(pltpu.VMEM((w, f, SLOTS), F32) for _ in range(2) for w, f in zip(WINDOW, (4, 4, 1))),
            *(pltpu.VMEM((2, ROWS, w, f, SLOTS), F32) for w, f in zip(WIDTH, (4, 4, 1))),
            pltpu.VMEM((WINDOW[0], 4, SLOTS), F32),
            pltpu.VMEM((COLS + 2, 1, SLOTS), F32),
            pltpu.VMEM((ROWS + 3, (COLS + 4) * SLOTS, 64), BF16),
            pltpu.VMEM((ROWS, COLS, 64, SLOTS), BF16),
            pltpu.VMEM((COLS + 2, 64, SLOTS), BF16),
            pltpu.VMEM((ROWS + 2, 64, (COLS + 2) * SLOTS), BF16),
            pltpu.VMEM((ROWS + 3, (COLS + 4) * SLOTS, SLOTS), F32),
            pltpu.VMEM(table, BF16),
            pltpu.VMEM(table, BF16),
            pltpu.VMEM(table, BF16),
            pltpu.VMEM((ROWS, COLS, 8, SLOTS), F32),
            pltpu.VMEM((ROWS, COLS, 24, SLOTS), F32),
            pltpu.SMEM((ROWS, COLS), jnp.int32),
            pltpu.VMEM((ROWS, 3, COLS, SLOTS), F32),
            pltpu.VMEM((ROWS, 3, COLS, SLOTS), F32),
            pltpu.VMEM((ROWS, COLS, SLOTS), F32),
            pltpu.SemaphoreType.DMA((4, 8)),
            pltpu.SemaphoreType.DMA((4, 8)),
            pltpu.SemaphoreType.DMA((4,)),
        ],
        compiler_params=pltpu.CompilerParams(
            collective_id=0, has_side_effects=True, vmem_limit_bytes=48 * 1024 * 1024
        ),
        name="sph_step",
    )(in_hbm(cell_counts), shear_shift, in_hbm(pos), in_hbm(vel), in_hbm(particle_mass))
    return density, jnp.transpose(accel, (0, 2, 3, 1))


def solution(mesh):
    placed = (
        P("gy", "gx", None, None),
        P("gy", "gx", None, None),
        P("gy", "gx", None),
        P("gy", "gx"),
        P(),
    )
    return jax.shard_map(
        functools.partial(local, mesh.shape["gy"], mesh.shape["gx"]),
        mesh=mesh,
        in_specs=placed,
        out_specs=(P("gy", "gx", None), P("gy", "gx", None, None)),
        check_vma=False,
    )
```

```python
import functools
import math

import jax
import jax.numpy as jnp
from jax import lax
from jax.experimental import pallas as pl
from jax.experimental.pallas import tpu as pltpu
from jax.sharding import PartitionSpec as P

SMOOTHING = 0.5
KERNEL_NORM = 1.0 / (math.pi * SMOOTHING**3)
SOUND_SQ = 0.2
VISCOSITY = 0.05
SOFTENING = 0.0025
SHEAR_JUMP = 1.0

MESH = pl.DeviceIdType.MESH
F32 = jnp.float32
BF16 = jnp.bfloat16
RHO_SCALE = KERNEL_NORM * 0.25
GRAD_SCALE = KERNEL_NORM * 0.75 / (SMOOTHING * SMOOTHING)
SOFT_Q = SOFTENING / (SMOOTHING * SMOOTHING)
TINY_Q = 1e-8
SLOTS = 128
ROWS = 2
COLS = 8
WIDTH = (2, 1, 1)
DRIFT = 4
EDGE = tuple(w + DRIFT for w in WIDTH)
WINDOW = tuple(2 * e + COLS for e in EDGE)
FAR = 3
EXTRA = 4


def pieces(p):
    high = p.astype(BF16).astype(F32)
    rest = p - high
    middle = rest.astype(BF16).astype(F32)
    return high, middle, rest - middle


def zeros(n):
    return jnp.zeros((n, SLOTS), F32)


def kernel(
    ny, nx,
    counts_in, shift, pos_in, vel_in, mass_in,
    dens_out, acc_out,
    own_a, own_v, own_m,
    below_a, below_v, below_m,
    above_a, above_v, above_m,
    side_a, side_v, side_m,
    far_a, far_m,
    near, centre, far_centre, feats, mass_cols,
    g_high, g_low, e_part,
    rho_part, sums,
    counts, pos, vel, mass,
    send_sem, recv_sem, load_sem,
):
    gy, gx = lax.axis_index("gy"), lax.axis_index("gx")
    top = gy // (ny - 1)
    bottom = (ny - 1 - gy) // (ny - 1)
    half = nx // 2
    up_y, down_y = lax.rem(gy + 1, ny), lax.rem(gy + ny - 1, ny)

    def up_id(k):
        return (up_y, lax.rem(gx + half * top + k + nx, nx))

    def down_id(k):
        return (down_y, lax.rem(gx + half * bottom + k + nx, nx))

    left_id = (gy, lax.rem(gx + nx - 1, nx))
    right_id = (gy, lax.rem(gx + 1, nx))

    row_a, row_v, row_m = (below_a, above_a), (below_v, above_v), (below_m, above_m)
    barrier = pltpu.get_barrier_semaphore()
    for k in (0, -1, 1):
        pl.semaphore_signal(barrier, inc=1, device_id=up_id(k), device_id_type=MESH)
        pl.semaphore_signal(barrier, inc=1, device_id=down_id(k), device_id_type=MESH)
    pl.semaphore_signal(barrier, inc=1, device_id=left_id, device_id_type=MESH)
    pl.semaphore_signal(barrier, inc=1, device_id=right_id, device_id_type=MESH)

    loads = [
        pltpu.make_async_copy(src, dst, load_sem.at[i])
        for i, (src, dst) in enumerate(
            ((counts_in, counts), (pos_in, pos), (mass_in, mass), (vel_in, vel))
        )
    ]
    for load in loads:
        load.start()

    def copy_of(phase, slot, src, dst, device):
        return pltpu.make_async_remote_copy(
            src_ref=src,
            dst_ref=dst,
            send_sem=send_sem.at[phase, slot],
            recv_sem=recv_sem.at[phase, slot],
            device_id=device,
            device_id_type=MESH,
        )

    def spans(edge):
        return ((1, COLS - edge, edge, 0), (0, 0, COLS, edge), (-1, 0, edge, edge + COLS))

    def row_copies(phase, slot, src, dst, device):
        return [
            copy_of(phase, slot - k, src.at[pl.ds(start, count)], dst.at[pl.ds(at, count)], device(k))
            for k, start, count, at in spans(EDGE[phase % FAR])
        ]

    def up_copies(phase, own, row):
        return row_copies(phase, 1, own.at[1], row[0], up_id)

    def down_copies(phase, own, row):
        return row_copies(phase, 4, own.at[0], row[1], down_id)

    def side_copies(phase, own, side):
        w = WIDTH[phase]
        return [
            copy_of(phase, 6, own.at[:, pl.ds(COLS - w, w)], side.at[0], right_id),
            copy_of(phase, 7, own.at[:, pl.ds(0, w)], side.at[1], left_id),
        ]

    def far_copies():
        return (
            row_copies(FAR, 1, own_a.at[0], far_a, up_id),
            row_copies(FAR, 1, own_a.at[1], far_a, down_id),
        )

    def start(copies):
        for copy in copies:
            copy.start()

    def wait_row(phase, own, row, d):
        for copy in row_copies(phase, 3 * d + 1, own.at[0], row[d], lambda k: left_id):
            copy.wait_recv()

    def wait_side(phase, own, side):
        for copy in side_copies(phase, own, side):
            copy.wait_recv()

    spot = lax.broadcasted_iota(jnp.int32, (64, SLOTS), 0)
    pick_mass = ((spot == 5) | (spot == 29) | (spot == 45)).astype(F32).astype(BF16)
    lane = lax.broadcasted_iota(jnp.int32, (COLS, SLOTS), 1)
    column = lax.broadcasted_iota(jnp.int32, (COLS, SLOTS), 0).astype(F32)

    def valid_of(r):
        bound = jnp.concatenate([jnp.full((1, SLOTS), counts[r, c], jnp.int32) for c in range(COLS)], axis=0)
        return lane < bound

    for load in loads:
        load.wait()
    for r in range(ROWS):
        fields = [pos[r, 0], pos[r, 1], pos[r, 2], jnp.where(valid_of(r), mass[r], 0.0)]
        for f in range(4):
            for c in range(COLS):
                own_a[r, c, f : f + 1, :] = fields[f][c : c + 1, :]
        for f in range(3):
            for c in range(COLS):
                own_v[r, c, f : f + 1, :] = vel[r, f][c : c + 1, :]
        for c in range(COLS):
            own_v[r, c, 3:4, :] = zeros(1)

    def scaled(xyzw, j, row):
        row = row.astype(F32) if hasattr(row, "astype") else float(row)
        x = 2.0 * xyzw[0:1] + (2.0 * j - 10.0)
        y = 2.0 * xyzw[1:2] + (2.0 * row - 4.0)
        return x, y, 2.0 * xyzw[2:3] - 1.0

    def prepare(e, j, xyzw, row=None):
        x, y, z = scaled(xyzw, j, e if row is None else row)
        w = xyzw[3:4]
        n = x * x + y * y + z * z
        lhs = jnp.concatenate([x, y, z, n, jnp.ones((1, SLOTS), F32), w, zeros(2)], axis=0)
        high, middle, low = pieces(lhs)
        table = jnp.concatenate([high, high, high, middle, middle, low, zeros(16)], axis=0).T
        at = (j + 1) * SLOTS
        near[e, at : at + SLOTS, :] = table.astype(BF16)
        mass_cols[e, at : at + SLOTS, :] = jnp.dot(table.astype(BF16), pick_mass, preferred_element_type=F32)
        if row is None and 0 <= j < COLS + 2:
            first = jnp.concatenate([w, w * x, w * y, w * z, zeros(4)], axis=0)
            feats[e, 32:64, j * SLOTS : (j + 1) * SLOTS] = jnp.concatenate([*pieces(first), zeros(8)], axis=0).astype(BF16)

    def centre_of(xyzw, j, row):
        x, y, z = scaled(xyzw, j, row)
        n = x * x + y * y + z * z
        rhs = jnp.concatenate([-2.0 * x, -2.0 * y, -2.0 * z, jnp.ones((1, SLOTS), F32), n, zeros(3)], axis=0)
        high, middle, low = pieces(rhs)
        return jnp.concatenate([high, middle, low, high, middle, high, zeros(16)], axis=0).astype(BF16)

    def prepare_own(r, carry):
        for c in range(COLS):
            prepare(r + 1, c + 1, own_a[r, c])
            centre[r, c] = centre_of(own_a[r, c], c + 1, r + 1)
        return carry

    sent_a = up_copies(0, own_a, row_a) + down_copies(0, own_a, row_a) + side_copies(0, own_a, side_a)
    sent_v = up_copies(1, own_v, row_v) + down_copies(1, own_v, row_v) + side_copies(1, own_v, side_v)
    sent_up, sent_down = far_copies()

    def exchange():
        pl.semaphore_wait(barrier, 8)
        start(sent_a)
        pl.when(top == 1)(lambda: start(sent_up))
        pl.when(bottom == 1)(lambda: start(sent_down))
        start(sent_v)

    patient = (top + bottom) * (1 - gx // half)
    pl.when(patient == 0)(exchange)
    lax.fori_loop(0, ROWS, prepare_own, 0)
    rho_part[...] = jnp.zeros_like(rho_part)
    sums[...] = jnp.zeros_like(sums)

    def kernel_of(cells, rhs):
        q_sq = jnp.maximum(jnp.dot(cells, rhs, preferred_element_type=F32), TINY_Q)
        inverse = lax.rsqrt(q_sq)
        q = q_sq * inverse
        u = jnp.maximum(2.0 - q, 0.0)
        s = jnp.maximum(1.0 - q, 0.0)
        u_sq = u * u
        s_sq = 4.0 * (s * s)
        return u_sq * u - s_sq * s, (s_sq - u_sq) * inverse, q_sq

    def pairs(r, a, c):
        e = r + a
        total = rho_part[r, c]
        rhs = centre[r, c]
        for b in range(3):
            at = (c + b + 1) * SLOTS
            value, slope, q_sq = kernel_of(near[e, at : at + SLOTS, :], rhs)
            soft = lax.rsqrt(q_sq + SOFT_Q)
            extra = (slope * soft) * soft
            weighted = value * mass_cols[e, at : at + SLOTS, :]
            total = total + jnp.sum(weighted.reshape(SLOTS // 8, 8, SLOTS), axis=0)
            high = slope.astype(BF16)
            span = pl.ds(b * SLOTS, SLOTS)
            g_high[r, a, c, span, :] = high
            g_low[r, a, c, span, :] = (slope - high.astype(F32)).astype(BF16)
            e_part[r, a, c, span, :] = extra.astype(BF16)
        rho_part[r, c] = total

    def reduce(r, a, c):
        e = r + a
        lanes = pl.ds(c * SLOTS, 3 * SLOTS)
        rows = feats[e, :, lanes]
        g = jnp.dot(rows, g_high[r, a, c], preferred_element_type=F32)
        g = g + jnp.dot(rows, g_low[r, a, c], preferred_element_type=F32)
        v = jnp.dot(rows[0:32], e_part[r, a, c], preferred_element_type=F32)
        sums[r, c, 0:8, :] += g[0:8] + g[8:16] + g[16:24]
        sums[r, c, 8:16, :] += g[32:40] + g[40:48] + g[48:56]
        sums[r, c, 16:24, :] += v[0:8] + v[8:16] + v[16:24]

    def own_units(work, cells):
        def body(t, carry):
            r = t // 2
            a = 1 - r + lax.rem(t, 2)
            for c in cells:
                work(r, a, c)
            return carry

        lax.fori_loop(0, 4, body, 0)

    inner, outer = tuple(range(1, COLS - 1)), (0, COLS - 1)
    own_units(pairs, inner)
    drift = jnp.clip(shift[0] - half * COLS, -DRIFT, DRIFT)
    drifts = (bottom * drift, -top * drift)
    far_side = (bottom, top)

    def window(phase, d, j):
        return EDGE[phase] - 1 + drifts[d] + j

    def near_row(work):
        pl.when(bottom == 1)(lambda: work(1))
        pl.when(bottom == 0)(lambda: work(0))

    def last_row(work):
        pl.when(bottom == 1)(lambda: work(0))
        pl.when(bottom == 0)(lambda: work(1))

    def ghost_pairs(d):
        wait_row(0, own_a, row_a, d)
        for j in range(COLS + 2):
            prepare(3 * d, j, row_a[d][window(0, d, j)])
        for c in range(COLS):
            pairs(d, 2 * d, c)

    near_row(ghost_pairs)
    pl.when(patient == 1)(exchange)
    wait_side(0, own_a, side_a)
    for s in (0, 1):
        for r in range(ROWS):
            prepare(r + 1, (COLS + 1) * s, side_a[s, r, 1 - s])
    own_units(pairs, outer)

    last_row(ghost_pairs)

    valid = [valid_of(r) for r in range(ROWS)]
    inverse_rho = []
    for r in range(ROWS):
        rho = jnp.concatenate([jnp.sum(rho_part[r, c], axis=0, keepdims=True) for c in range(COLS)], axis=0) * RHO_SCALE
        dens_out[r] = jnp.where(valid[r], rho, 0.0)
        inv = 1.0 / jnp.where(valid[r], rho, 1.0)
        inverse_rho.append(inv)
        ratio = jnp.where(valid[r], mass[r], 0.0) * inv
        for c in range(COLS):
            own_m[r, c] = ratio[c : c + 1, :]
    sent_m = up_copies(2, own_m, row_m), down_copies(2, own_m, row_m), side_copies(2, own_m, side_m)
    pl.when(top == 0)(lambda: start(sent_m[0]))
    pl.when(bottom == 0)(lambda: start(sent_m[1]))
    start(sent_m[2])

    def far_tables(d):
        for copy in row_copies(FAR, 1, own_a.at[0], far_a, lambda k: left_id):
            copy.wait_recv()
        for j in range(-1, COLS + 3):
            prepare(EXTRA, j, far_a[window(0, d, j)], row=5 * d - 1)
        for s in (0, 1):
            j = (COLS + 3) * s - 1
            prepare(3 * d, j, row_a[d][window(0, d, j)])
            prepare(d + 1, j, side_a[s, d, s])
        for j in range(COLS + 2):
            far_centre[j] = centre_of(row_a[d][window(0, d, j)], j, 3 * d)

    def far_density(d):
        def body(t, carry):
            for i in range(5):
                j = 5 * t + i
                total = zeros(8)
                rhs = far_centre[j]
                for n, e in enumerate((d + 1, 3 * d, EXTRA)):
                    for b in range(3):
                        at = pl.multiple_of((j + b) * SLOTS, SLOTS)
                        value, _, _ = kernel_of(near[e, pl.ds(at, SLOTS), :], rhs)
                        weighted = value * mass_cols[e, pl.ds(at, SLOTS), :]
                        total = total + jnp.sum(weighted.reshape(SLOTS // 8, 8, SLOTS), axis=0)
                    turn = 3 * i + n
                    if turn < 2 * len(inner):
                        reduce(t, 1 - t + turn // len(inner), inner[turn % len(inner)])
                far_m[j] = jnp.sum(total, axis=0, keepdims=True) * RHO_SCALE
            return carry

        lax.fori_loop(0, 2, body, 0)

    def second(e, j, xyzw, v, ratio, jump):
        x, y, z = scaled(xyzw, j, e)
        block = jnp.concatenate(
            [ratio, ratio * x, ratio * y, ratio * z, ratio * (v[0:1] + jump), ratio * v[1:2], ratio * v[2:3], zeros(1)],
            axis=0,
        )
        feats[e, 0:32, j * SLOTS : (j + 1) * SLOTS] = jnp.concatenate([*pieces(block), zeros(8)], axis=0).astype(BF16)

    def second_own(r, carry):
        for c in range(COLS):
            second(r + 1, c + 1, own_a[r, c], own_v[r, c], own_m[r, c], 0.0)
        return carry

    lax.fori_loop(0, ROWS, second_own, 0)
    pl.when(bottom == 1)(lambda: far_tables(0))
    pl.when(top == 1)(lambda: far_tables(1))
    pl.when(bottom + top == 1)(lambda: far_density(top))
    pl.when(bottom + top == 0)(lambda: own_units(reduce, inner))
    wait_side(1, own_v, side_v)
    wait_side(2, own_m, side_m)
    for s in (0, 1):
        for r in range(ROWS):
            second(r + 1, (COLS + 1) * s, side_a[s, r, 1 - s], side_v[s, r, 0], side_m[s, r, 0], 0.0)
    own_units(reduce, outer)

    jumps = (-(bottom.astype(F32)) * SHEAR_JUMP, top.astype(F32) * SHEAR_JUMP)

    def ghost_reduce(d):
        wait_row(1, own_v, row_v, d)
        pl.when(far_side[d] == 0)(lambda: wait_row(2, own_m, row_m, d))
        for j in range(COLS + 2):
            xyzw = row_a[d][window(0, d, j)]
            w = xyzw[3:4]
            far_ratio = w / jnp.where(w > 0.0, far_m[j], 1.0)
            ratio = jnp.where(far_side[d] == 1, far_ratio, row_m[d][window(2, d, j)])
            second(3 * d, j, xyzw, row_v[d][window(1, d, j)], ratio, jumps[d])
        for c in range(COLS):
            reduce(d, 2 * d, c)

    near_row(ghost_reduce)
    last_row(ghost_reduce)

    for r in range(ROWS):
        def row_of(k):
            return jnp.concatenate([sums[r, c, k : k + 1, :] for c in range(COLS)], axis=0)

        block = [
            2.0 * pos[r, 0] + (2.0 * column - 8.0),
            2.0 * pos[r, 1] + (2.0 * r - 2.0),
            2.0 * pos[r, 2] - 1.0,
        ]
        inv = inverse_rho[r]
        ratio_sum, mass_sum = row_of(0), row_of(8)
        visc_sum = ratio_sum - SOFT_Q * row_of(16)
        for f in range(3):
            far = block[f] * ratio_sum - row_of(1 + f)
            near_part = block[f] * mass_sum - row_of(9 + f)
            drag = vel[r, f] * visc_sum - (row_of(4 + f) - SOFT_Q * row_of(20 + f))
            total = (-0.5 * SOUND_SQ * GRAD_SCALE) * (inv * near_part + far) + (2.0 * VISCOSITY * GRAD_SCALE) * (inv * drag)
            acc_out[r, f] = jnp.where(valid[r], total, 0.0)

    def drain(copies):
        for copy in copies:
            copy.wait_send()

    drain(sent_a + sent_v + sent_m[2])
    pl.when(top == 1)(lambda: drain(sent_up))
    pl.when(top == 0)(lambda: drain(sent_m[0]))
    pl.when(bottom == 1)(lambda: drain(sent_down))
    pl.when(bottom == 0)(lambda: drain(sent_m[1]))


def local(ny, nx, position, velocity, particle_mass, cell_counts, shear_shift):
    pos = jnp.transpose(position, (0, 3, 1, 2))
    vel = jnp.transpose(velocity, (0, 3, 1, 2))
    vmem = pl.BlockSpec(memory_space=pltpu.VMEM)
    hbm = pl.BlockSpec(memory_space=pltpu.HBM)
    in_hbm = functools.partial(pltpu.with_memory_space_constraint, memory_space=pltpu.HBM)
    table = (ROWS, 3, COLS, 3 * SLOTS, SLOTS)
    density, accel = pl.pallas_call(
        functools.partial(kernel, ny, nx),
        out_shape=(
            jax.ShapeDtypeStruct((ROWS, COLS, SLOTS), F32),
            jax.ShapeDtypeStruct((ROWS, 3, COLS, SLOTS), F32),
        ),
        in_specs=[hbm, pl.BlockSpec(memory_space=pltpu.SMEM), hbm, hbm, hbm],
        out_specs=(vmem, vmem),
        scratch_shapes=[
            pltpu.VMEM((ROWS, COLS, 4, SLOTS), F32),
            pltpu.VMEM((ROWS, COLS, 4, SLOTS), F32),
            pltpu.VMEM((ROWS, COLS, 1, SLOTS), F32),
            *(pltpu.VMEM((w, f, SLOTS), F32) for _ in range(2) for w, f in zip(WINDOW, (4, 4, 1))),
            *(pltpu.VMEM((2, ROWS, w, f, SLOTS), F32) for w, f in zip(WIDTH, (4, 4, 1))),
            pltpu.VMEM((WINDOW[0], 4, SLOTS), F32),
            pltpu.VMEM((COLS + 2, 1, SLOTS), F32),
            pltpu.VMEM((ROWS + 3, (COLS + 4) * SLOTS, 64), BF16),
            pltpu.VMEM((ROWS, COLS, 64, SLOTS), BF16),
            pltpu.VMEM((COLS + 2, 64, SLOTS), BF16),
            pltpu.VMEM((ROWS + 2, 64, (COLS + 2) * SLOTS), BF16),
            pltpu.VMEM((ROWS + 3, (COLS + 4) * SLOTS, SLOTS), F32),
            pltpu.VMEM(table, BF16),
            pltpu.VMEM(table, BF16),
            pltpu.VMEM(table, BF16),
            pltpu.VMEM((ROWS, COLS, 8, SLOTS), F32),
            pltpu.VMEM((ROWS, COLS, 24, SLOTS), F32),
            pltpu.SMEM((ROWS, COLS), jnp.int32),
            pltpu.VMEM((ROWS, 3, COLS, SLOTS), F32),
            pltpu.VMEM((ROWS, 3, COLS, SLOTS), F32),
            pltpu.VMEM((ROWS, COLS, SLOTS), F32),
            pltpu.SemaphoreType.DMA((4, 8)),
            pltpu.SemaphoreType.DMA((4, 8)),
            pltpu.SemaphoreType.DMA((4,)),
        ],
        compiler_params=pltpu.CompilerParams(
            collective_id=0, has_side_effects=True, vmem_limit_bytes=48 * 1024 * 1024
        ),
        name="sph_step",
    )(in_hbm(cell_counts), shear_shift, in_hbm(pos), in_hbm(vel), in_hbm(particle_mass))
    return density, jnp.transpose(accel, (0, 2, 3, 1))


def solution(mesh):
    placed = (
        P("gy", "gx", None, None),
        P("gy", "gx", None, None),
        P("gy", "gx", None),
        P("gy", "gx"),
        P(),
    )
    return jax.shard_map(
        functools.partial(local, mesh.shape["gy"], mesh.shape["gx"]),
        mesh=mesh,
        in_specs=placed,
        out_specs=(P("gy", "gx", None), P("gy", "gx", None, None)),
        check_vma=False,
    )
```

```python
import functools
import math

import jax
import jax.numpy as jnp
from jax import lax
from jax.experimental import pallas as pl
from jax.experimental.pallas import tpu as pltpu
from jax.sharding import PartitionSpec as P

SMOOTHING = 0.5
KERNEL_NORM = 1.0 / (math.pi * SMOOTHING**3)
SOUND_SQ = 0.2
VISCOSITY = 0.05
SOFTENING = 0.0025
SHEAR_JUMP = 1.0

MESH = pl.DeviceIdType.MESH
F32 = jnp.float32
BF16 = jnp.bfloat16
RHO_SCALE = KERNEL_NORM * 0.25
GRAD_SCALE = KERNEL_NORM * 0.75 / (SMOOTHING * SMOOTHING)
SOFT_Q = SOFTENING / (SMOOTHING * SMOOTHING)
TINY_Q = 1e-8
SLOTS = 128
ROWS = 2
COLS = 8
WIDTH = (2, 1, 1)
DRIFT = 4
EDGE = tuple(w + DRIFT for w in WIDTH)
WINDOW = tuple(2 * e + COLS for e in EDGE)
FAR = 3
EXTRA = 4


def pieces(p):
    high = p.astype(BF16).astype(F32)
    rest = p - high
    middle = rest.astype(BF16).astype(F32)
    return high, middle, rest - middle


def zeros(n):
    return jnp.zeros((n, SLOTS), F32)


def kernel(
    ny, nx,
    counts_in, shift, pos_in, vel_in, mass_in,
    dens_out, acc_out,
    own_a, own_v, own_m,
    below_a, below_v, below_m,
    above_a, above_v, above_m,
    side_a, side_v, side_m,
    far_a, far_m,
    near, centre, far_centre, feats, mass_cols,
    g_high, g_low, e_part,
    rho_part, sums,
    counts, pos, vel, mass,
    send_sem, recv_sem, load_sem,
):
    gy, gx = lax.axis_index("gy"), lax.axis_index("gx")
    top = gy // (ny - 1)
    bottom = (ny - 1 - gy) // (ny - 1)
    half = nx // 2
    up_y, down_y = lax.rem(gy + 1, ny), lax.rem(gy + ny - 1, ny)

    def up_id(k):
        return (up_y, lax.rem(gx + half * top + k + nx, nx))

    def down_id(k):
        return (down_y, lax.rem(gx + half * bottom + k + nx, nx))

    left_id = (gy, lax.rem(gx + nx - 1, nx))
    right_id = (gy, lax.rem(gx + 1, nx))

    row_a, row_v, row_m = (below_a, above_a), (below_v, above_v), (below_m, above_m)
    barrier = pltpu.get_barrier_semaphore()
    for k in (0, -1, 1):
        pl.semaphore_signal(barrier, inc=1, device_id=up_id(k), device_id_type=MESH)
        pl.semaphore_signal(barrier, inc=1, device_id=down_id(k), device_id_type=MESH)
    pl.semaphore_signal(barrier, inc=1, device_id=left_id, device_id_type=MESH)
    pl.semaphore_signal(barrier, inc=1, device_id=right_id, device_id_type=MESH)

    loads = [
        pltpu.make_async_copy(src, dst, load_sem.at[i])
        for i, (src, dst) in enumerate(
            ((counts_in, counts), (pos_in, pos), (mass_in, mass), (vel_in, vel))
        )
    ]
    for load in loads:
        load.start()

    def copy_of(phase, slot, src, dst, device):
        return pltpu.make_async_remote_copy(
            src_ref=src,
            dst_ref=dst,
            send_sem=send_sem.at[phase, slot],
            recv_sem=recv_sem.at[phase, slot],
            device_id=device,
            device_id_type=MESH,
        )

    def spans(edge):
        return ((1, COLS - edge, edge, 0), (0, 0, COLS, edge), (-1, 0, edge, edge + COLS))

    def row_copies(phase, slot, src, dst, device):
        return [
            copy_of(phase, slot - k, src.at[pl.ds(start, count)], dst.at[pl.ds(at, count)], device(k))
            for k, start, count, at in spans(EDGE[phase % FAR])
        ]

    def up_copies(phase, own, row):
        return row_copies(phase, 1, own.at[1], row[0], up_id)

    def down_copies(phase, own, row):
        return row_copies(phase, 4, own.at[0], row[1], down_id)

    def side_copies(phase, own, side):
        w = WIDTH[phase]
        return [
            copy_of(phase, 6, own.at[:, pl.ds(COLS - w, w)], side.at[0], right_id),
            copy_of(phase, 7, own.at[:, pl.ds(0, w)], side.at[1], left_id),
        ]

    def far_copies():
        return (
            row_copies(FAR, 1, own_a.at[0], far_a, up_id),
            row_copies(FAR, 1, own_a.at[1], far_a, down_id),
        )

    def start(copies):
        for copy in copies:
            copy.start()

    def wait_row(phase, own, row, d):
        for copy in row_copies(phase, 3 * d + 1, own.at[0], row[d], lambda k: left_id):
            copy.wait_recv()

    def wait_side(phase, own, side):
        for copy in side_copies(phase, own, side):
            copy.wait_recv()

    spot = lax.broadcasted_iota(jnp.int32, (64, SLOTS), 0)
    pick_mass = ((spot == 5) | (spot == 29) | (spot == 45)).astype(F32).astype(BF16)
    lane = lax.broadcasted_iota(jnp.int32, (COLS, SLOTS), 1)
    column = lax.broadcasted_iota(jnp.int32, (COLS, SLOTS), 0).astype(F32)

    def valid_of(r):
        bound = jnp.concatenate([jnp.full((1, SLOTS), counts[r, c], jnp.int32) for c in range(COLS)], axis=0)
        return lane < bound

    for load in loads:
        load.wait()
    for r in range(ROWS):
        fields = [pos[r, 0], pos[r, 1], pos[r, 2], jnp.where(valid_of(r), mass[r], 0.0)]
        for f in range(4):
            for c in range(COLS):
                own_a[r, c, f : f + 1, :] = fields[f][c : c + 1, :]
        for f in range(3):
            for c in range(COLS):
                own_v[r, c, f : f + 1, :] = vel[r, f][c : c + 1, :]
        for c in range(COLS):
            own_v[r, c, 3:4, :] = zeros(1)

    def scaled(xyzw, j, row):
        row = row.astype(F32) if hasattr(row, "astype") else float(row)
        x = 2.0 * xyzw[0:1] + (2.0 * j - 10.0)
        y = 2.0 * xyzw[1:2] + (2.0 * row - 4.0)
        return x, y, 2.0 * xyzw[2:3] - 1.0

    def prepare(e, j, xyzw, row=None):
        x, y, z = scaled(xyzw, j, e if row is None else row)
        w = xyzw[3:4]
        n = x * x + y * y + z * z
        lhs = jnp.concatenate([x, y, z, n, jnp.ones((1, SLOTS), F32), w, zeros(2)], axis=0)
        high, middle, low = pieces(lhs)
        table = jnp.concatenate([high, high, high, middle, middle, low, zeros(16)], axis=0).T
        at = (j + 1) * SLOTS
        near[e, at : at + SLOTS, :] = table.astype(BF16)
        mass_cols[e, at : at + SLOTS, :] = jnp.dot(table.astype(BF16), pick_mass, preferred_element_type=F32)
        if row is None and 0 <= j < COLS + 2:
            first = jnp.concatenate([w, w * x, w * y, w * z, zeros(4)], axis=0)
            feats[e, 32:64, j * SLOTS : (j + 1) * SLOTS] = jnp.concatenate([*pieces(first), zeros(8)], axis=0).astype(BF16)

    def centre_of(xyzw, j, row):
        x, y, z = scaled(xyzw, j, row)
        n = x * x + y * y + z * z
        rhs = jnp.concatenate([-2.0 * x, -2.0 * y, -2.0 * z, jnp.ones((1, SLOTS), F32), n, zeros(3)], axis=0)
        high, middle, low = pieces(rhs)
        return jnp.concatenate([high, middle, low, high, middle, high, zeros(16)], axis=0).astype(BF16)

    def prepare_own(r, carry):
        for c in range(COLS):
            prepare(r + 1, c + 1, own_a[r, c])
            centre[r, c] = centre_of(own_a[r, c], c + 1, r + 1)
        return carry

    sent_a = up_copies(0, own_a, row_a) + down_copies(0, own_a, row_a) + side_copies(0, own_a, side_a)
    sent_v = up_copies(1, own_v, row_v) + down_copies(1, own_v, row_v) + side_copies(1, own_v, side_v)
    sent_up, sent_down = far_copies()

    def exchange():
        pl.semaphore_wait(barrier, 8)
        start(sent_a)
        pl.when(top == 1)(lambda: start(sent_up))
        pl.when(bottom == 1)(lambda: start(sent_down))
        start(sent_v)

    first = (nx - gx) // nx
    patient = jnp.maximum((top + bottom) * (1 - gx // half), first)
    pl.when(patient == 0)(exchange)
    lax.fori_loop(0, ROWS, prepare_own, 0)
    rho_part[...] = jnp.zeros_like(rho_part)
    sums[...] = jnp.zeros_like(sums)

    def kernel_of(cells, rhs):
        q_sq = jnp.maximum(jnp.dot(cells, rhs, preferred_element_type=F32), TINY_Q)
        inverse = lax.rsqrt(q_sq)
        q = q_sq * inverse
        u = jnp.maximum(2.0 - q, 0.0)
        s = jnp.maximum(1.0 - q, 0.0)
        u_sq = u * u
        s_sq = 4.0 * (s * s)
        return u_sq * u - s_sq * s, (s_sq - u_sq) * inverse, q_sq

    def pairs(r, a, c):
        e = r + a
        total = rho_part[r, c]
        rhs = centre[r, c]
        for b in range(3):
            at = (c + b + 1) * SLOTS
            value, slope, q_sq = kernel_of(near[e, at : at + SLOTS, :], rhs)
            soft = lax.rsqrt(q_sq + SOFT_Q)
            extra = (slope * soft) * soft
            weighted = value * mass_cols[e, at : at + SLOTS, :]
            total = total + jnp.sum(weighted.reshape(SLOTS // 8, 8, SLOTS), axis=0)
            high = slope.astype(BF16)
            span = pl.ds(b * SLOTS, SLOTS)
            g_high[r, a, c, span, :] = high
            g_low[r, a, c, span, :] = (slope - high.astype(F32)).astype(BF16)
            e_part[r, a, c, span, :] = extra.astype(BF16)
        rho_part[r, c] = total

    def reduce(r, a, c):
        e = r + a
        lanes = pl.ds(c * SLOTS, 3 * SLOTS)
        rows = feats[e, :, lanes]
        g = jnp.dot(rows, g_high[r, a, c], preferred_element_type=F32)
        g = g + jnp.dot(rows, g_low[r, a, c], preferred_element_type=F32)
        v = jnp.dot(rows[0:32], e_part[r, a, c], preferred_element_type=F32)
        sums[r, c, 0:8, :] += g[0:8] + g[8:16] + g[16:24]
        sums[r, c, 8:16, :] += g[32:40] + g[40:48] + g[48:56]
        sums[r, c, 16:24, :] += v[0:8] + v[8:16] + v[16:24]

    def own_units(work, cells):
        def body(t, carry):
            r = t // 2
            a = 1 - r + lax.rem(t, 2)
            for c in cells:
                work(r, a, c)
            return carry

        lax.fori_loop(0, 4, body, 0)

    inner, outer = tuple(range(1, COLS - 1)), (0, COLS - 1)
    own_units(pairs, inner)
    drift = jnp.clip(shift[0] - half * COLS, -DRIFT, DRIFT)
    drifts = (bottom * drift, -top * drift)
    far_side = (bottom, top)

    def window(phase, d, j):
        return EDGE[phase] - 1 + drifts[d] + j

    def near_row(work):
        pl.when(bottom == 1)(lambda: work(1))
        pl.when(bottom == 0)(lambda: work(0))

    def last_row(work):
        pl.when(bottom == 1)(lambda: work(0))
        pl.when(bottom == 0)(lambda: work(1))

    def ghost_pairs(d):
        wait_row(0, own_a, row_a, d)
        for j in range(COLS + 2):
            prepare(3 * d, j, row_a[d][window(0, d, j)])
        for c in range(COLS):
            pairs(d, 2 * d, c)

    pl.when(patient == 1)(exchange)
    wait_side(0, own_a, side_a)
    for s in (0, 1):
        for r in range(ROWS):
            prepare(r + 1, (COLS + 1) * s, side_a[s, r, 1 - s])
    own_units(pairs, outer)

    near_row(ghost_pairs)
    last_row(ghost_pairs)

    valid = [valid_of(r) for r in range(ROWS)]
    inverse_rho = []
    for r in range(ROWS):
        rho = jnp.concatenate([jnp.sum(rho_part[r, c], axis=0, keepdims=True) for c in range(COLS)], axis=0) * RHO_SCALE
        dens_out[r] = jnp.where(valid[r], rho, 0.0)
        inv = 1.0 / jnp.where(valid[r], rho, 1.0)
        inverse_rho.append(inv)
        ratio = jnp.where(valid[r], mass[r], 0.0) * inv
        for c in range(COLS):
            own_m[r, c] = ratio[c : c + 1, :]
    sent_m = up_copies(2, own_m, row_m), down_copies(2, own_m, row_m), side_copies(2, own_m, side_m)
    pl.when(top == 0)(lambda: start(sent_m[0]))
    pl.when(bottom == 0)(lambda: start(sent_m[1]))
    start(sent_m[2])

    def far_tables(d):
        for copy in row_copies(FAR, 1, own_a.at[0], far_a, lambda k: left_id):
            copy.wait_recv()
        for j in range(-1, COLS + 3):
            prepare(EXTRA, j, far_a[window(0, d, j)], row=5 * d - 1)
        for s in (0, 1):
            j = (COLS + 3) * s - 1
            prepare(3 * d, j, row_a[d][window(0, d, j)])
            prepare(d + 1, j, side_a[s, d, s])
        for j in range(COLS + 2):
            far_centre[j] = centre_of(row_a[d][window(0, d, j)], j, 3 * d)

    def far_density(d):
        def body(t, carry):
            for i in range(5):
                j = 5 * t + i
                total = zeros(8)
                rhs = far_centre[j]
                for n, e in enumerate((d + 1, 3 * d, EXTRA)):
                    for b in range(3):
                        at = pl.multiple_of((j + b) * SLOTS, SLOTS)
                        value, _, _ = kernel_of(near[e, pl.ds(at, SLOTS), :], rhs)
                        weighted = value * mass_cols[e, pl.ds(at, SLOTS), :]
                        total = total + jnp.sum(weighted.reshape(SLOTS // 8, 8, SLOTS), axis=0)
                    turn = 3 * i + n
                    if turn < 2 * len(inner):
                        reduce(t, 1 - t + turn // len(inner), inner[turn % len(inner)])
                far_m[j] = jnp.sum(total, axis=0, keepdims=True) * RHO_SCALE
            return carry

        lax.fori_loop(0, 2, body, 0)

    def second(e, j, xyzw, v, ratio, jump):
        x, y, z = scaled(xyzw, j, e)
        block = jnp.concatenate(
            [ratio, ratio * x, ratio * y, ratio * z, ratio * (v[0:1] + jump), ratio * v[1:2], ratio * v[2:3], zeros(1)],
            axis=0,
        )
        feats[e, 0:32, j * SLOTS : (j + 1) * SLOTS] = jnp.concatenate([*pieces(block), zeros(8)], axis=0).astype(BF16)

    def second_own(r, carry):
        for c in range(COLS):
            second(r + 1, c + 1, own_a[r, c], own_v[r, c], own_m[r, c], 0.0)
        return carry

    lax.fori_loop(0, ROWS, second_own, 0)
    pl.when(bottom == 1)(lambda: far_tables(0))
    pl.when(top == 1)(lambda: far_tables(1))
    pl.when(bottom + top == 1)(lambda: far_density(top))
    pl.when(bottom + top == 0)(lambda: own_units(reduce, inner))
    wait_side(1, own_v, side_v)
    wait_side(2, own_m, side_m)
    for s in (0, 1):
        for r in range(ROWS):
            second(r + 1, (COLS + 1) * s, side_a[s, r, 1 - s], side_v[s, r, 0], side_m[s, r, 0], 0.0)
    own_units(reduce, outer)

    jumps = (-(bottom.astype(F32)) * SHEAR_JUMP, top.astype(F32) * SHEAR_JUMP)

    def ghost_reduce(d):
        wait_row(1, own_v, row_v, d)
        pl.when(far_side[d] == 0)(lambda: wait_row(2, own_m, row_m, d))
        for j in range(COLS + 2):
            xyzw = row_a[d][window(0, d, j)]
            w = xyzw[3:4]
            far_ratio = w / jnp.where(w > 0.0, far_m[j], 1.0)
            ratio = jnp.where(far_side[d] == 1, far_ratio, row_m[d][window(2, d, j)])
            second(3 * d, j, xyzw, row_v[d][window(1, d, j)], ratio, jumps[d])
        for c in range(COLS):
            reduce(d, 2 * d, c)

    near_row(ghost_reduce)
    last_row(ghost_reduce)

    for r in range(ROWS):
        def row_of(k):
            return jnp.concatenate([sums[r, c, k : k + 1, :] for c in range(COLS)], axis=0)

        block = [
            2.0 * pos[r, 0] + (2.0 * column - 8.0),
            2.0 * pos[r, 1] + (2.0 * r - 2.0),
            2.0 * pos[r, 2] - 1.0,
        ]
        inv = inverse_rho[r]
        ratio_sum, mass_sum = row_of(0), row_of(8)
        visc_sum = ratio_sum - SOFT_Q * row_of(16)
        for f in range(3):
            far = block[f] * ratio_sum - row_of(1 + f)
            near_part = block[f] * mass_sum - row_of(9 + f)
            drag = vel[r, f] * visc_sum - (row_of(4 + f) - SOFT_Q * row_of(20 + f))
            total = (-0.5 * SOUND_SQ * GRAD_SCALE) * (inv * near_part + far) + (2.0 * VISCOSITY * GRAD_SCALE) * (inv * drag)
            acc_out[r, f] = jnp.where(valid[r], total, 0.0)

    def drain(copies):
        for copy in copies:
            copy.wait_send()

    drain(sent_a + sent_v + sent_m[2])
    pl.when(top == 1)(lambda: drain(sent_up))
    pl.when(top == 0)(lambda: drain(sent_m[0]))
    pl.when(bottom == 1)(lambda: drain(sent_down))
    pl.when(bottom == 0)(lambda: drain(sent_m[1]))


def local(ny, nx, position, velocity, particle_mass, cell_counts, shear_shift):
    pos = jnp.transpose(position, (0, 3, 1, 2))
    vel = jnp.transpose(velocity, (0, 3, 1, 2))
    vmem = pl.BlockSpec(memory_space=pltpu.VMEM)
    hbm = pl.BlockSpec(memory_space=pltpu.HBM)
    in_hbm = functools.partial(pltpu.with_memory_space_constraint, memory_space=pltpu.HBM)
    table = (ROWS, 3, COLS, 3 * SLOTS, SLOTS)
    density, accel = pl.pallas_call(
        functools.partial(kernel, ny, nx),
        out_shape=(
            jax.ShapeDtypeStruct((ROWS, COLS, SLOTS), F32),
            jax.ShapeDtypeStruct((ROWS, 3, COLS, SLOTS), F32),
        ),
        in_specs=[hbm, pl.BlockSpec(memory_space=pltpu.SMEM), hbm, hbm, hbm],
        out_specs=(vmem, vmem),
        scratch_shapes=[
            pltpu.VMEM((ROWS, COLS, 4, SLOTS), F32),
            pltpu.VMEM((ROWS, COLS, 4, SLOTS), F32),
            pltpu.VMEM((ROWS, COLS, 1, SLOTS), F32),
            *(pltpu.VMEM((w, f, SLOTS), F32) for _ in range(2) for w, f in zip(WINDOW, (4, 4, 1))),
            *(pltpu.VMEM((2, ROWS, w, f, SLOTS), F32) for w, f in zip(WIDTH, (4, 4, 1))),
            pltpu.VMEM((WINDOW[0], 4, SLOTS), F32),
            pltpu.VMEM((COLS + 2, 1, SLOTS), F32),
            pltpu.VMEM((ROWS + 3, (COLS + 4) * SLOTS, 64), BF16),
            pltpu.VMEM((ROWS, COLS, 64, SLOTS), BF16),
            pltpu.VMEM((COLS + 2, 64, SLOTS), BF16),
            pltpu.VMEM((ROWS + 2, 64, (COLS + 2) * SLOTS), BF16),
            pltpu.VMEM((ROWS + 3, (COLS + 4) * SLOTS, SLOTS), F32),
            pltpu.VMEM(table, BF16),
            pltpu.VMEM(table, BF16),
            pltpu.VMEM(table, BF16),
            pltpu.VMEM((ROWS, COLS, 8, SLOTS), F32),
            pltpu.VMEM((ROWS, COLS, 24, SLOTS), F32),
            pltpu.SMEM((ROWS, COLS), jnp.int32),
            pltpu.VMEM((ROWS, 3, COLS, SLOTS), F32),
            pltpu.VMEM((ROWS, 3, COLS, SLOTS), F32),
            pltpu.VMEM((ROWS, COLS, SLOTS), F32),
            pltpu.SemaphoreType.DMA((4, 8)),
            pltpu.SemaphoreType.DMA((4, 8)),
            pltpu.SemaphoreType.DMA((4,)),
        ],
        compiler_params=pltpu.CompilerParams(
            collective_id=0, has_side_effects=True, vmem_limit_bytes=48 * 1024 * 1024
        ),
        name="sph_step",
    )(in_hbm(cell_counts), shear_shift, in_hbm(pos), in_hbm(vel), in_hbm(particle_mass))
    return density, jnp.transpose(accel, (0, 2, 3, 1))


def solution(mesh):
    placed = (
        P("gy", "gx", None, None),
        P("gy", "gx", None, None),
        P("gy", "gx", None),
        P("gy", "gx"),
        P(),
    )
    return jax.shard_map(
        functools.partial(local, mesh.shape["gy"], mesh.shape["gx"]),
        mesh=mesh,
        in_specs=placed,
        out_specs=(P("gy", "gx", None), P("gy", "gx", None, None)),
        check_vma=False,
    )
```

```python
import functools
import math

import jax
import jax.numpy as jnp
from jax import lax
from jax.experimental import pallas as pl
from jax.experimental.pallas import tpu as pltpu
from jax.sharding import PartitionSpec as P

SMOOTHING = 0.5
KERNEL_NORM = 1.0 / (math.pi * SMOOTHING**3)
SOUND_SQ = 0.2
VISCOSITY = 0.05
SOFTENING = 0.0025
SHEAR_JUMP = 1.0

MESH = pl.DeviceIdType.MESH
F32 = jnp.float32
BF16 = jnp.bfloat16
RHO_SCALE = KERNEL_NORM * 0.25
GRAD_SCALE = KERNEL_NORM * 0.75 / (SMOOTHING * SMOOTHING)
SOFT_Q = SOFTENING / (SMOOTHING * SMOOTHING)
TINY_Q = 1e-8
SLOTS = 128
ROWS = 2
COLS = 8
WIDTH = (2, 1, 1)
DRIFT = 4
EDGE = (WIDTH[0] + DRIFT, WIDTH[1] + DRIFT, 1)
WINDOW = tuple(2 * e + COLS for e in EDGE)
FAR = 3
EXTRA = 4


def pieces(p):
    high = p.astype(BF16).astype(F32)
    rest = p - high
    middle = rest.astype(BF16).astype(F32)
    return high, middle, rest - middle


def zeros(n):
    return jnp.zeros((n, SLOTS), F32)


def kernel(
    ny, nx,
    counts_in, shift, pos_in, vel_in, mass_in,
    dens_out, acc_out,
    own_a, own_v, own_m,
    below_a, below_v, below_m,
    above_a, above_v, above_m,
    side_a, side_v, side_m,
    far_a, far_m,
    near, centre, far_centre, feats, mass_cols,
    g_high, g_low, e_part,
    rho_part, sums,
    counts, pos, vel, mass,
    send_sem, recv_sem, load_sem,
):
    gy, gx = lax.axis_index("gy"), lax.axis_index("gx")
    top = gy // (ny - 1)
    bottom = (ny - 1 - gy) // (ny - 1)
    half = nx // 2
    up_y, down_y = lax.rem(gy + 1, ny), lax.rem(gy + ny - 1, ny)

    def up_id(k):
        return (up_y, lax.rem(gx + half * top + k + nx, nx))

    def down_id(k):
        return (down_y, lax.rem(gx + half * bottom + k + nx, nx))

    left_id = (gy, lax.rem(gx + nx - 1, nx))
    right_id = (gy, lax.rem(gx + 1, nx))

    row_a, row_v, row_m = (below_a, above_a), (below_v, above_v), (below_m, above_m)
    barrier = pltpu.get_barrier_semaphore()
    for k in (0, -1, 1):
        pl.semaphore_signal(barrier, inc=1, device_id=up_id(k), device_id_type=MESH)
        pl.semaphore_signal(barrier, inc=1, device_id=down_id(k), device_id_type=MESH)
    pl.semaphore_signal(barrier, inc=1, device_id=left_id, device_id_type=MESH)
    pl.semaphore_signal(barrier, inc=1, device_id=right_id, device_id_type=MESH)

    loads = [
        pltpu.make_async_copy(src, dst, load_sem.at[i])
        for i, (src, dst) in enumerate(
            ((counts_in, counts), (pos_in, pos), (mass_in, mass), (vel_in, vel))
        )
    ]
    for load in loads:
        load.start()

    def copy_of(phase, slot, src, dst, device):
        return pltpu.make_async_remote_copy(
            src_ref=src,
            dst_ref=dst,
            send_sem=send_sem.at[phase, slot],
            recv_sem=recv_sem.at[phase, slot],
            device_id=device,
            device_id_type=MESH,
        )

    def spans(edge):
        return ((0, 0, COLS, edge), (1, COLS - edge, edge, 0), (-1, 0, edge, edge + COLS))

    def row_copies(phase, slot, src, dst, device):
        return [
            copy_of(phase, slot - k, src.at[pl.ds(start, count)], dst.at[pl.ds(at, count)], device(k))
            for k, start, count, at in spans(EDGE[phase % FAR])
        ]

    def up_copies(phase, own, row):
        return row_copies(phase, 1, own.at[1], row[0], up_id)

    def down_copies(phase, own, row):
        return row_copies(phase, 4, own.at[0], row[1], down_id)

    def side_copies(phase, own, side):
        w = WIDTH[phase]
        return [
            copy_of(phase, 6, own.at[:, pl.ds(COLS - w, w)], side.at[0], right_id),
            copy_of(phase, 7, own.at[:, pl.ds(0, w)], side.at[1], left_id),
        ]

    def far_copies():
        return (
            row_copies(FAR, 1, own_a.at[0], far_a, up_id),
            row_copies(FAR, 1, own_a.at[1], far_a, down_id),
        )

    def start(copies):
        for copy in copies:
            copy.start()

    def wait_row(phase, own, row, d):
        for copy in row_copies(phase, 3 * d + 1, own.at[0], row[d], lambda k: left_id):
            copy.wait_recv()

    def wait_side(phase, own, side):
        for copy in side_copies(phase, own, side):
            copy.wait_recv()

    spot = lax.broadcasted_iota(jnp.int32, (64, SLOTS), 0)
    pick_mass = ((spot == 5) | (spot == 29) | (spot == 45)).astype(F32).astype(BF16)
    lane = lax.broadcasted_iota(jnp.int32, (COLS, SLOTS), 1)
    column = lax.broadcasted_iota(jnp.int32, (COLS, SLOTS), 0).astype(F32)

    def valid_of(r):
        bound = jnp.concatenate([jnp.full((1, SLOTS), counts[r, c], jnp.int32) for c in range(COLS)], axis=0)
        return lane < bound

    for load in loads:
        load.wait()
    for r in range(ROWS):
        fields = [pos[r, 0], pos[r, 1], pos[r, 2], jnp.where(valid_of(r), mass[r], 0.0)]
        for f in range(4):
            for c in range(COLS):
                own_a[r, c, f : f + 1, :] = fields[f][c : c + 1, :]
        for f in range(3):
            for c in range(COLS):
                own_v[r, c, f : f + 1, :] = vel[r, f][c : c + 1, :]
        for c in range(COLS):
            own_v[r, c, 3:4, :] = zeros(1)

    def scaled(xyzw, j, row):
        row = row.astype(F32) if hasattr(row, "astype") else float(row)
        x = 2.0 * xyzw[0:1] + (2.0 * j - 10.0)
        y = 2.0 * xyzw[1:2] + (2.0 * row - 4.0)
        return x, y, 2.0 * xyzw[2:3] - 1.0

    def prepare(e, j, xyzw, row=None):
        x, y, z = scaled(xyzw, j, e if row is None else row)
        w = xyzw[3:4]
        n = x * x + y * y + z * z
        lhs = jnp.concatenate([x, y, z, n, jnp.ones((1, SLOTS), F32), w, zeros(2)], axis=0)
        high, middle, low = pieces(lhs)
        table = jnp.concatenate([high, high, high, middle, middle, low, zeros(16)], axis=0).T
        at = (j + 1) * SLOTS
        near[e, at : at + SLOTS, :] = table.astype(BF16)
        mass_cols[e, at : at + SLOTS, :] = jnp.dot(table.astype(BF16), pick_mass, preferred_element_type=F32)
        if row is None and 0 <= j < COLS + 2:
            first = jnp.concatenate([w, w * x, w * y, w * z, zeros(4)], axis=0)
            feats[e, 32:64, j * SLOTS : (j + 1) * SLOTS] = jnp.concatenate([*pieces(first), zeros(8)], axis=0).astype(BF16)

    def centre_of(xyzw, j, row):
        x, y, z = scaled(xyzw, j, row)
        n = x * x + y * y + z * z
        rhs = jnp.concatenate([-2.0 * x, -2.0 * y, -2.0 * z, jnp.ones((1, SLOTS), F32), n, zeros(3)], axis=0)
        high, middle, low = pieces(rhs)
        return jnp.concatenate([high, middle, low, high, middle, high, zeros(16)], axis=0).astype(BF16)

    def prepare_own(r, carry):
        for c in range(COLS):
            prepare(r + 1, c + 1, own_a[r, c])
            centre[r, c] = centre_of(own_a[r, c], c + 1, r + 1)
        return carry

    sent_a = up_copies(0, own_a, row_a) + down_copies(0, own_a, row_a) + side_copies(0, own_a, side_a)
    sent_v = up_copies(1, own_v, row_v) + down_copies(1, own_v, row_v) + side_copies(1, own_v, side_v)
    sent_up, sent_down = far_copies()

    def exchange():
        pl.semaphore_wait(barrier, 8)
        start(sent_a)
        pl.when(top == 1)(lambda: start(sent_up))
        pl.when(bottom == 1)(lambda: start(sent_down))
        start(sent_v)

    first = (nx - gx) // nx
    patient = jnp.maximum((top + bottom) * (1 - gx // half), first)
    pl.when(patient == 0)(exchange)
    lax.fori_loop(0, ROWS, prepare_own, 0)
    rho_part[...] = jnp.zeros_like(rho_part)
    sums[...] = jnp.zeros_like(sums)

    def kernel_of(cells, rhs):
        q_sq = jnp.maximum(jnp.dot(cells, rhs, preferred_element_type=F32), TINY_Q)
        inverse = lax.rsqrt(q_sq)
        q = q_sq * inverse
        u = jnp.maximum(2.0 - q, 0.0)
        s = jnp.maximum(1.0 - q, 0.0)
        u_sq = u * u
        s_sq = 4.0 * (s * s)
        return u_sq * u - s_sq * s, (s_sq - u_sq) * inverse, q_sq

    def pairs(r, a, c):
        e = r + a
        total = rho_part[r, c]
        rhs = centre[r, c]
        for b in range(3):
            at = (c + b + 1) * SLOTS
            value, slope, q_sq = kernel_of(near[e, at : at + SLOTS, :], rhs)
            soft = lax.rsqrt(q_sq + SOFT_Q)
            extra = (slope * soft) * soft
            weighted = value * mass_cols[e, at : at + SLOTS, :]
            total = total + jnp.sum(weighted.reshape(SLOTS // 8, 8, SLOTS), axis=0)
            high = slope.astype(BF16)
            span = pl.ds(b * SLOTS, SLOTS)
            g_high[r, a, c, span, :] = high
            g_low[r, a, c, span, :] = (slope - high.astype(F32)).astype(BF16)
            e_part[r, a, c, span, :] = extra.astype(BF16)
        rho_part[r, c] = total

    def reduce(r, a, c):
        e = r + a
        lanes = pl.ds(c * SLOTS, 3 * SLOTS)
        rows = feats[e, :, lanes]
        g = jnp.dot(rows, g_high[r, a, c], preferred_element_type=F32)
        g = g + jnp.dot(rows, g_low[r, a, c], preferred_element_type=F32)
        v = jnp.dot(rows[0:32], e_part[r, a, c], preferred_element_type=F32)
        sums[r, c, 0:8, :] += g[0:8] + g[8:16] + g[16:24]
        sums[r, c, 8:16, :] += g[32:40] + g[40:48] + g[48:56]
        sums[r, c, 16:24, :] += v[0:8] + v[8:16] + v[16:24]

    def own_units(work, cells):
        def body(t, carry):
            r = t // 2
            a = 1 - r + lax.rem(t, 2)
            for c in cells:
                work(r, a, c)
            return carry

        lax.fori_loop(0, 4, body, 0)

    inner, outer = tuple(range(1, COLS - 1)), (0, COLS - 1)
    own_units(pairs, inner)
    drift = jnp.clip(shift[0] - half * COLS, -DRIFT, DRIFT)
    drifts = (bottom * drift, -top * drift)
    far_side = (bottom, top)

    def window(phase, d, j):
        return EDGE[phase] - 1 + drifts[d] + j

    def near_row(work):
        pl.when(bottom == 1)(lambda: work(1))
        pl.when(bottom == 0)(lambda: work(0))

    def last_row(work):
        pl.when(bottom == 1)(lambda: work(0))
        pl.when(bottom == 0)(lambda: work(1))

    def ghost_first(d):
        wait_row(0, own_a, row_a, d)
        for j in range(COLS + 2):
            prepare(3 * d, j, row_a[d][window(0, d, j)])
        for c in outer:
            pairs(d, 2 * d, c)

    def ghost_rest(d):
        for c in inner:
            pairs(d, 2 * d, c)

    pl.when(patient == 1)(exchange)
    wait_side(0, own_a, side_a)
    for s in (0, 1):
        for r in range(ROWS):
            prepare(r + 1, (COLS + 1) * s, side_a[s, r, 1 - s])
    own_units(pairs, outer)

    edge = top + bottom
    near_row(ghost_first)
    pl.when(edge == 1)(lambda: ghost_rest(bottom))
    last_row(ghost_first)

    sent_m = up_copies(2, own_m, row_m), down_copies(2, own_m, row_m), side_copies(2, own_m, side_m)
    for r in range(ROWS):
        for c in outer:
            rho = jnp.sum(rho_part[r, c], axis=0, keepdims=True) * RHO_SCALE
            own_m[r, c] = own_a[r, c][3:4] / jnp.where(lane[0:1] < counts[r, c], rho, 1.0)
    start(sent_m[2])
    pl.when(top == 0)(lambda: start(sent_m[0][1:]))
    pl.when(bottom == 0)(lambda: start(sent_m[1][1:]))

    def rest(t, carry):
        ghost_rest(edge * top + (1 - edge) * t)
        return carry

    lax.fori_loop(edge, 2, rest, 0)

    valid = [valid_of(r) for r in range(ROWS)]
    inverse_rho = []
    for r in range(ROWS):
        rho = jnp.concatenate([jnp.sum(rho_part[r, c], axis=0, keepdims=True) for c in range(COLS)], axis=0) * RHO_SCALE
        dens_out[r] = jnp.where(valid[r], rho, 0.0)
        inv = 1.0 / jnp.where(valid[r], rho, 1.0)
        inverse_rho.append(inv)
        ratio = jnp.where(valid[r], mass[r], 0.0) * inv
        for c in inner:
            own_m[r, c] = ratio[c : c + 1, :]
    pl.when(top == 0)(lambda: start(sent_m[0][:1]))
    pl.when(bottom == 0)(lambda: start(sent_m[1][:1]))

    def far_tables(d):
        for copy in row_copies(FAR, 1, own_a.at[0], far_a, lambda k: left_id):
            copy.wait_recv()
        for j in range(-1, COLS + 3):
            prepare(EXTRA, j, far_a[window(0, d, j)], row=5 * d - 1)
        for s in (0, 1):
            j = (COLS + 3) * s - 1
            prepare(3 * d, j, row_a[d][window(0, d, j)])
            prepare(d + 1, j, side_a[s, d, s])
        for j in range(COLS + 2):
            far_centre[j] = centre_of(row_a[d][window(0, d, j)], j, 3 * d)

    def far_density(d):
        def body(t, carry):
            for i in range(5):
                j = 5 * t + i
                total = zeros(8)
                rhs = far_centre[j]
                for n, e in enumerate((d + 1, 3 * d, EXTRA)):
                    for b in range(3):
                        at = pl.multiple_of((j + b) * SLOTS, SLOTS)
                        value, _, _ = kernel_of(near[e, pl.ds(at, SLOTS), :], rhs)
                        weighted = value * mass_cols[e, pl.ds(at, SLOTS), :]
                        total = total + jnp.sum(weighted.reshape(SLOTS // 8, 8, SLOTS), axis=0)
                    turn = 3 * i + n
                    if turn < 2 * len(inner):
                        reduce(t, 1 - t + turn // len(inner), inner[turn % len(inner)])
                far_m[j] = jnp.sum(total, axis=0, keepdims=True) * RHO_SCALE
            return carry

        lax.fori_loop(0, 2, body, 0)

    def second(e, j, xyzw, v, ratio, jump):
        x, y, z = scaled(xyzw, j, e)
        block = jnp.concatenate(
            [ratio, ratio * x, ratio * y, ratio * z, ratio * (v[0:1] + jump), ratio * v[1:2], ratio * v[2:3], zeros(1)],
            axis=0,
        )
        feats[e, 0:32, j * SLOTS : (j + 1) * SLOTS] = jnp.concatenate([*pieces(block), zeros(8)], axis=0).astype(BF16)

    def second_own(r, carry):
        for c in range(COLS):
            second(r + 1, c + 1, own_a[r, c], own_v[r, c], own_m[r, c], 0.0)
        return carry

    lax.fori_loop(0, ROWS, second_own, 0)
    pl.when(bottom == 1)(lambda: far_tables(0))
    pl.when(top == 1)(lambda: far_tables(1))
    pl.when(edge == 1)(lambda: far_density(top))
    pl.when(edge == 0)(lambda: own_units(reduce, inner))
    wait_side(1, own_v, side_v)
    wait_side(2, own_m, side_m)
    for s in (0, 1):
        for r in range(ROWS):
            second(r + 1, (COLS + 1) * s, side_a[s, r, 1 - s], side_v[s, r, 0], side_m[s, r, 0], 0.0)
    own_units(reduce, outer)

    jumps = (-(bottom.astype(F32)) * SHEAR_JUMP, top.astype(F32) * SHEAR_JUMP)

    def ghost_reduce(d):
        wait_row(1, own_v, row_v, d)
        pl.when(far_side[d] == 0)(lambda: wait_row(2, own_m, row_m, d))
        for j in range(COLS + 2):
            xyzw = row_a[d][window(0, d, j)]
            w = xyzw[3:4]
            far_ratio = w / jnp.where(w > 0.0, far_m[j], 1.0)
            ratio = jnp.where(far_side[d] == 1, far_ratio, row_m[d][j])
            second(3 * d, j, xyzw, row_v[d][window(1, d, j)], ratio, jumps[d])
        for c in range(COLS):
            reduce(d, 2 * d, c)

    near_row(ghost_reduce)
    last_row(ghost_reduce)

    for r in range(ROWS):
        def row_of(k):
            return jnp.concatenate([sums[r, c, k : k + 1, :] for c in range(COLS)], axis=0)

        block = [
            2.0 * pos[r, 0] + (2.0 * column - 8.0),
            2.0 * pos[r, 1] + (2.0 * r - 2.0),
            2.0 * pos[r, 2] - 1.0,
        ]
        inv = inverse_rho[r]
        ratio_sum, mass_sum = row_of(0), row_of(8)
        visc_sum = ratio_sum - SOFT_Q * row_of(16)
        for f in range(3):
            far = block[f] * ratio_sum - row_of(1 + f)
            near_part = block[f] * mass_sum - row_of(9 + f)
            drag = vel[r, f] * visc_sum - (row_of(4 + f) - SOFT_Q * row_of(20 + f))
            total = (-0.5 * SOUND_SQ * GRAD_SCALE) * (inv * near_part + far) + (2.0 * VISCOSITY * GRAD_SCALE) * (inv * drag)
            acc_out[r, f] = jnp.where(valid[r], total, 0.0)

    def drain(copies):
        for copy in copies:
            copy.wait_send()

    drain(sent_a + sent_v + sent_m[2])
    pl.when(top == 1)(lambda: drain(sent_up))
    pl.when(top == 0)(lambda: drain(sent_m[0]))
    pl.when(bottom == 1)(lambda: drain(sent_down))
    pl.when(bottom == 0)(lambda: drain(sent_m[1]))


def local(ny, nx, position, velocity, particle_mass, cell_counts, shear_shift):
    pos = jnp.transpose(position, (0, 3, 1, 2))
    vel = jnp.transpose(velocity, (0, 3, 1, 2))
    vmem = pl.BlockSpec(memory_space=pltpu.VMEM)
    hbm = pl.BlockSpec(memory_space=pltpu.HBM)
    in_hbm = functools.partial(pltpu.with_memory_space_constraint, memory_space=pltpu.HBM)
    table = (ROWS, 3, COLS, 3 * SLOTS, SLOTS)
    density, accel = pl.pallas_call(
        functools.partial(kernel, ny, nx),
        out_shape=(
            jax.ShapeDtypeStruct((ROWS, COLS, SLOTS), F32),
            jax.ShapeDtypeStruct((ROWS, 3, COLS, SLOTS), F32),
        ),
        in_specs=[hbm, pl.BlockSpec(memory_space=pltpu.SMEM), hbm, hbm, hbm],
        out_specs=(vmem, vmem),
        scratch_shapes=[
            pltpu.VMEM((ROWS, COLS, 4, SLOTS), F32),
            pltpu.VMEM((ROWS, COLS, 4, SLOTS), F32),
            pltpu.VMEM((ROWS, COLS, 1, SLOTS), F32),
            *(pltpu.VMEM((w, f, SLOTS), F32) for _ in range(2) for w, f in zip(WINDOW, (4, 4, 1))),
            *(pltpu.VMEM((2, ROWS, w, f, SLOTS), F32) for w, f in zip(WIDTH, (4, 4, 1))),
            pltpu.VMEM((WINDOW[0], 4, SLOTS), F32),
            pltpu.VMEM((COLS + 2, 1, SLOTS), F32),
            pltpu.VMEM((ROWS + 3, (COLS + 4) * SLOTS, 64), BF16),
            pltpu.VMEM((ROWS, COLS, 64, SLOTS), BF16),
            pltpu.VMEM((COLS + 2, 64, SLOTS), BF16),
            pltpu.VMEM((ROWS + 2, 64, (COLS + 2) * SLOTS), BF16),
            pltpu.VMEM((ROWS + 3, (COLS + 4) * SLOTS, SLOTS), F32),
            pltpu.VMEM(table, BF16),
            pltpu.VMEM(table, BF16),
            pltpu.VMEM(table, BF16),
            pltpu.VMEM((ROWS, COLS, 8, SLOTS), F32),
            pltpu.VMEM((ROWS, COLS, 24, SLOTS), F32),
            pltpu.SMEM((ROWS, COLS), jnp.int32),
            pltpu.VMEM((ROWS, 3, COLS, SLOTS), F32),
            pltpu.VMEM((ROWS, 3, COLS, SLOTS), F32),
            pltpu.VMEM((ROWS, COLS, SLOTS), F32),
            pltpu.SemaphoreType.DMA((4, 8)),
            pltpu.SemaphoreType.DMA((4, 8)),
            pltpu.SemaphoreType.DMA((4,)),
        ],
        compiler_params=pltpu.CompilerParams(
            collective_id=0, has_side_effects=True, vmem_limit_bytes=48 * 1024 * 1024
        ),
        name="sph_step",
    )(in_hbm(cell_counts), shear_shift, in_hbm(pos), in_hbm(vel), in_hbm(particle_mass))
    return density, jnp.transpose(accel, (0, 2, 3, 1))


def solution(mesh):
    placed = (
        P("gy", "gx", None, None),
        P("gy", "gx", None, None),
        P("gy", "gx", None),
        P("gy", "gx"),
        P(),
    )
    return jax.shard_map(
        functools.partial(local, mesh.shape["gy"], mesh.shape["gx"]),
        mesh=mesh,
        in_specs=placed,
        out_specs=(P("gy", "gx", None), P("gy", "gx", None, None)),
        check_vma=False,
    )
```

```python
import functools
import math

import jax
import jax.numpy as jnp
from jax import lax
from jax.experimental import pallas as pl
from jax.experimental.pallas import tpu as pltpu
from jax.sharding import PartitionSpec as P

SMOOTHING = 0.5
KERNEL_NORM = 1.0 / (math.pi * SMOOTHING**3)
SOUND_SQ = 0.2
VISCOSITY = 0.05
SOFTENING = 0.0025
SHEAR_JUMP = 1.0

MESH = pl.DeviceIdType.MESH
F32 = jnp.float32
BF16 = jnp.bfloat16
RHO_SCALE = KERNEL_NORM * 0.25
GRAD_SCALE = KERNEL_NORM * 0.75 / (SMOOTHING * SMOOTHING)
SOFT_Q = SOFTENING / (SMOOTHING * SMOOTHING)
TINY_Q = 1e-8
SLOTS = 128
ROWS = 2
COLS = 8
WIDTH = (2, 1, 1)
DRIFT = 4
EDGE = (WIDTH[0] + DRIFT, WIDTH[1] + DRIFT, 1)
WINDOW = tuple(2 * e + COLS for e in EDGE)
FAR = 3
EXTRA = 4


def pieces(p):
    high = p.astype(BF16).astype(F32)
    rest = p - high
    middle = rest.astype(BF16).astype(F32)
    return high, middle, rest - middle


def zeros(n):
    return jnp.zeros((n, SLOTS), F32)


def kernel(
    ny, nx,
    counts_in, shift, pos_in, vel_in, mass_in,
    dens_out, acc_out,
    own_a, own_v, own_m,
    below_a, below_v, below_m,
    above_a, above_v, above_m,
    side_a, side_v, side_m,
    far_a, far_m,
    near, centre, far_centre, feats, mass_cols,
    g_high, g_low, e_part,
    rho_part, sums,
    counts, pos, vel, mass,
    send_sem, recv_sem, load_sem,
):
    gy, gx = lax.axis_index("gy"), lax.axis_index("gx")
    top = gy // (ny - 1)
    bottom = (ny - 1 - gy) // (ny - 1)
    half = nx // 2
    up_y, down_y = lax.rem(gy + 1, ny), lax.rem(gy + ny - 1, ny)

    def up_id(k):
        return (up_y, lax.rem(gx + half * top + k + nx, nx))

    def down_id(k):
        return (down_y, lax.rem(gx + half * bottom + k + nx, nx))

    left_id = (gy, lax.rem(gx + nx - 1, nx))
    right_id = (gy, lax.rem(gx + 1, nx))

    row_a, row_v, row_m = (below_a, above_a), (below_v, above_v), (below_m, above_m)
    barrier = pltpu.get_barrier_semaphore()
    for k in (0, -1, 1):
        pl.semaphore_signal(barrier, inc=1, device_id=up_id(k), device_id_type=MESH)
        pl.semaphore_signal(barrier, inc=1, device_id=down_id(k), device_id_type=MESH)
    pl.semaphore_signal(barrier, inc=1, device_id=left_id, device_id_type=MESH)
    pl.semaphore_signal(barrier, inc=1, device_id=right_id, device_id_type=MESH)

    loads = [
        pltpu.make_async_copy(src, dst, load_sem.at[i])
        for i, (src, dst) in enumerate(
            ((counts_in, counts), (pos_in, pos), (mass_in, mass), (vel_in, vel))
        )
    ]
    for load in loads:
        load.start()

    def copy_of(phase, slot, src, dst, device):
        return pltpu.make_async_remote_copy(
            src_ref=src,
            dst_ref=dst,
            send_sem=send_sem.at[phase, slot],
            recv_sem=recv_sem.at[phase, slot],
            device_id=device,
            device_id_type=MESH,
        )

    def spans(edge):
        return ((0, 0, COLS, edge), (1, COLS - edge, edge, 0), (-1, 0, edge, edge + COLS))

    def row_copies(phase, slot, src, dst, device):
        return [
            copy_of(phase, slot - k, src.at[pl.ds(start, count)], dst.at[pl.ds(at, count)], device(k))
            for k, start, count, at in spans(EDGE[phase % FAR])
        ]

    def up_copies(phase, own, row):
        return row_copies(phase, 1, own.at[1], row[0], up_id)

    def down_copies(phase, own, row):
        return row_copies(phase, 4, own.at[0], row[1], down_id)

    def side_copies(phase, own, side):
        w = WIDTH[phase]
        return [
            copy_of(phase, 6, own.at[:, pl.ds(COLS - w, w)], side.at[0], right_id),
            copy_of(phase, 7, own.at[:, pl.ds(0, w)], side.at[1], left_id),
        ]

    def far_copies():
        return (
            row_copies(FAR, 1, own_a.at[0], far_a, up_id),
            row_copies(FAR, 1, own_a.at[1], far_a, down_id),
        )

    def start(copies):
        for copy in copies:
            copy.start()

    def wait_row(phase, own, row, d):
        for copy in row_copies(phase, 3 * d + 1, own.at[0], row[d], lambda k: left_id):
            copy.wait_recv()

    def wait_side(phase, own, side):
        for copy in side_copies(phase, own, side):
            copy.wait_recv()

    spot = lax.broadcasted_iota(jnp.int32, (64, SLOTS), 0)
    pick_mass = ((spot == 5) | (spot == 29) | (spot == 45)).astype(F32).astype(BF16)
    lane = lax.broadcasted_iota(jnp.int32, (COLS, SLOTS), 1)
    column = lax.broadcasted_iota(jnp.int32, (COLS, SLOTS), 0).astype(F32)

    def valid_of(r):
        bound = jnp.concatenate([jnp.full((1, SLOTS), counts[r, c], jnp.int32) for c in range(COLS)], axis=0)
        return lane < bound

    for load in loads:
        load.wait()
    for r in range(ROWS):
        fields = [pos[r, 0], pos[r, 1], pos[r, 2], jnp.where(valid_of(r), mass[r], 0.0)]
        for f in range(4):
            for c in range(COLS):
                own_a[r, c, f : f + 1, :] = fields[f][c : c + 1, :]
        for f in range(3):
            for c in range(COLS):
                own_v[r, c, f : f + 1, :] = vel[r, f][c : c + 1, :]
        for c in range(COLS):
            own_v[r, c, 3:4, :] = zeros(1)

    def scaled(xyzw, j, row):
        row = row.astype(F32) if hasattr(row, "astype") else float(row)
        x = 2.0 * xyzw[0:1] + (2.0 * j - 10.0)
        y = 2.0 * xyzw[1:2] + (2.0 * row - 4.0)
        return x, y, 2.0 * xyzw[2:3] - 1.0

    def prepare(e, j, xyzw, row=None):
        x, y, z = scaled(xyzw, j, e if row is None else row)
        w = xyzw[3:4]
        n = x * x + y * y + z * z
        lhs = jnp.concatenate([x, y, z, n, jnp.ones((1, SLOTS), F32), w, zeros(2)], axis=0)
        high, middle, low = pieces(lhs)
        table = jnp.concatenate([high, high, high, middle, middle, low, zeros(16)], axis=0).T
        at = (j + 1) * SLOTS
        near[e, at : at + SLOTS, :] = table.astype(BF16)
        mass_cols[e, at : at + SLOTS, :] = jnp.dot(table.astype(BF16), pick_mass, preferred_element_type=F32)
        if row is None and 0 <= j < COLS + 2:
            first = jnp.concatenate([w, w * x, w * y, w * z, zeros(4)], axis=0)
            feats[e, 32:64, j * SLOTS : (j + 1) * SLOTS] = jnp.concatenate([*pieces(first), zeros(8)], axis=0).astype(BF16)

    def centre_of(xyzw, j, row):
        x, y, z = scaled(xyzw, j, row)
        n = x * x + y * y + z * z
        rhs = jnp.concatenate([-2.0 * x, -2.0 * y, -2.0 * z, jnp.ones((1, SLOTS), F32), n, zeros(3)], axis=0)
        high, middle, low = pieces(rhs)
        return jnp.concatenate([high, middle, low, high, middle, high, zeros(16)], axis=0).astype(BF16)

    def prepare_own(r, carry):
        for c in range(COLS):
            prepare(r + 1, c + 1, own_a[r, c])
            centre[r, c] = centre_of(own_a[r, c], c + 1, r + 1)
        return carry

    sent_a = up_copies(0, own_a, row_a) + down_copies(0, own_a, row_a) + side_copies(0, own_a, side_a)
    sent_v = up_copies(1, own_v, row_v) + down_copies(1, own_v, row_v) + side_copies(1, own_v, side_v)
    sent_up, sent_down = far_copies()

    def exchange():
        pl.semaphore_wait(barrier, 8)
        start(sent_a)
        pl.when(top == 1)(lambda: start(sent_up))
        pl.when(bottom == 1)(lambda: start(sent_down))
        start(sent_v)

    first = (nx - gx) // nx
    patient = jnp.maximum((top + bottom) * (1 - gx // half), first)
    pl.when(patient == 0)(exchange)
    lax.fori_loop(0, ROWS, prepare_own, 0)
    rho_part[...] = jnp.zeros_like(rho_part)
    sums[...] = jnp.zeros_like(sums)

    def kernel_of(cells, rhs):
        q_sq = jnp.maximum(jnp.dot(cells, rhs, preferred_element_type=F32), TINY_Q)
        inverse = lax.rsqrt(q_sq)
        q = q_sq * inverse
        u = jnp.maximum(2.0 - q, 0.0)
        s = jnp.maximum(1.0 - q, 0.0)
        u_sq = u * u
        s_sq = 4.0 * (s * s)
        return u_sq * u - s_sq * s, (s_sq - u_sq) * inverse, q_sq

    def pairs(r, a, c):
        e = r + a
        total = rho_part[r, c]
        rhs = centre[r, c]
        for b in range(3):
            at = (c + b + 1) * SLOTS
            value, slope, q_sq = kernel_of(near[e, at : at + SLOTS, :], rhs)
            soft = lax.rsqrt(q_sq + SOFT_Q)
            extra = (slope * soft) * soft
            weighted = value * mass_cols[e, at : at + SLOTS, :]
            total = total + jnp.sum(weighted.reshape(SLOTS // 8, 8, SLOTS), axis=0)
            high = slope.astype(BF16)
            span = pl.ds(b * SLOTS, SLOTS)
            g_high[r, a, c, span, :] = high
            g_low[r, a, c, span, :] = (slope - high.astype(F32)).astype(BF16)
            e_part[r, a, c, span, :] = extra.astype(BF16)
        rho_part[r, c] = total

    def reduce(r, a, c):
        e = r + a
        lanes = pl.ds(c * SLOTS, 3 * SLOTS)
        rows = feats[e, :, lanes]
        g = jnp.dot(rows, g_high[r, a, c], preferred_element_type=F32)
        g = g + jnp.dot(rows, g_low[r, a, c], preferred_element_type=F32)
        v = jnp.dot(rows[0:32], e_part[r, a, c], preferred_element_type=F32)
        sums[r, c, 0:8, :] += g[0:8] + g[8:16] + g[16:24]
        sums[r, c, 8:16, :] += g[32:40] + g[40:48] + g[48:56]
        sums[r, c, 16:24, :] += v[0:8] + v[8:16] + v[16:24]

    def own_units(work, cells):
        def body(t, carry):
            r = t // 2
            a = 1 - r + lax.rem(t, 2)
            for c in cells:
                work(r, a, c)
            return carry

        lax.fori_loop(0, 4, body, 0)

    inner, outer = tuple(range(1, COLS - 1)), (0, COLS - 1)
    own_units(pairs, inner)
    drift = jnp.clip(shift[0] - half * COLS, -DRIFT, DRIFT)
    drifts = (bottom * drift, -top * drift)
    far_side = (bottom, top)

    def window(phase, d, j):
        return EDGE[phase] - 1 + drifts[d] + j

    def near_row(work):
        pl.when(bottom == 1)(lambda: work(1))
        pl.when(bottom == 0)(lambda: work(0))

    def last_row(work):
        pl.when(bottom == 1)(lambda: work(0))
        pl.when(bottom == 0)(lambda: work(1))

    def ghost_first(d):
        wait_row(0, own_a, row_a, d)
        for j in range(COLS + 2):
            prepare(3 * d, j, row_a[d][window(0, d, j)])
        for c in outer:
            pairs(d, 2 * d, c)

    def ghost_rest(d):
        for c in inner:
            pairs(d, 2 * d, c)

    pl.when(patient == 1)(exchange)

    edge = top + bottom
    near_row(ghost_first)
    pl.when(edge == 1)(lambda: ghost_rest(bottom))
    wait_side(0, own_a, side_a)
    for s in (0, 1):
        for r in range(ROWS):
            prepare(r + 1, (COLS + 1) * s, side_a[s, r, 1 - s])
    own_units(pairs, outer)
    last_row(ghost_first)

    sent_m = up_copies(2, own_m, row_m), down_copies(2, own_m, row_m), side_copies(2, own_m, side_m)
    for r in range(ROWS):
        for c in outer:
            rho = jnp.sum(rho_part[r, c], axis=0, keepdims=True) * RHO_SCALE
            own_m[r, c] = own_a[r, c][3:4] / jnp.where(lane[0:1] < counts[r, c], rho, 1.0)
    start(sent_m[2])
    pl.when(top == 0)(lambda: start(sent_m[0][1:]))
    pl.when(bottom == 0)(lambda: start(sent_m[1][1:]))

    def rest(t, carry):
        ghost_rest(edge * top + (1 - edge) * t)
        return carry

    lax.fori_loop(edge, 2, rest, 0)

    valid = [valid_of(r) for r in range(ROWS)]
    inverse_rho = []
    for r in range(ROWS):
        rho = jnp.concatenate([jnp.sum(rho_part[r, c], axis=0, keepdims=True) for c in range(COLS)], axis=0) * RHO_SCALE
        dens_out[r] = jnp.where(valid[r], rho, 0.0)
        inv = 1.0 / jnp.where(valid[r], rho, 1.0)
        inverse_rho.append(inv)
        ratio = jnp.where(valid[r], mass[r], 0.0) * inv
        for c in inner:
            own_m[r, c] = ratio[c : c + 1, :]
    pl.when(top == 0)(lambda: start(sent_m[0][:1]))
    pl.when(bottom == 0)(lambda: start(sent_m[1][:1]))

    def far_tables(d):
        for copy in row_copies(FAR, 1, own_a.at[0], far_a, lambda k: left_id):
            copy.wait_recv()
        for j in range(-1, COLS + 3):
            prepare(EXTRA, j, far_a[window(0, d, j)], row=5 * d - 1)
        for s in (0, 1):
            j = (COLS + 3) * s - 1
            prepare(3 * d, j, row_a[d][window(0, d, j)])
            prepare(d + 1, j, side_a[s, d, s])
        for j in range(COLS + 2):
            far_centre[j] = centre_of(row_a[d][window(0, d, j)], j, 3 * d)

    def far_density(d):
        def body(t, carry):
            for i in range(5):
                j = 5 * t + i
                total = zeros(8)
                rhs = far_centre[j]
                for n, e in enumerate((d + 1, 3 * d, EXTRA)):
                    for b in range(3):
                        at = pl.multiple_of((j + b) * SLOTS, SLOTS)
                        value, _, _ = kernel_of(near[e, pl.ds(at, SLOTS), :], rhs)
                        weighted = value * mass_cols[e, pl.ds(at, SLOTS), :]
                        total = total + jnp.sum(weighted.reshape(SLOTS // 8, 8, SLOTS), axis=0)
                    turn = 3 * i + n
                    if turn < 2 * len(inner):
                        reduce(t, 1 - t + turn // len(inner), inner[turn % len(inner)])
                far_m[j] = jnp.sum(total, axis=0, keepdims=True) * RHO_SCALE
            return carry

        lax.fori_loop(0, 2, body, 0)

    def second(e, j, xyzw, v, ratio, jump):
        x, y, z = scaled(xyzw, j, e)
        block = jnp.concatenate(
            [ratio, ratio * x, ratio * y, ratio * z, ratio * (v[0:1] + jump), ratio * v[1:2], ratio * v[2:3], zeros(1)],
            axis=0,
        )
        feats[e, 0:32, j * SLOTS : (j + 1) * SLOTS] = jnp.concatenate([*pieces(block), zeros(8)], axis=0).astype(BF16)

    def second_own(r, carry):
        for c in range(COLS):
            second(r + 1, c + 1, own_a[r, c], own_v[r, c], own_m[r, c], 0.0)
        return carry

    lax.fori_loop(0, ROWS, second_own, 0)
    pl.when(bottom == 1)(lambda: far_tables(0))
    pl.when(top == 1)(lambda: far_tables(1))
    pl.when(edge == 1)(lambda: far_density(top))
    pl.when(edge == 0)(lambda: own_units(reduce, inner))
    wait_side(1, own_v, side_v)
    wait_side(2, own_m, side_m)
    for s in (0, 1):
        for r in range(ROWS):
            second(r + 1, (COLS + 1) * s, side_a[s, r, 1 - s], side_v[s, r, 0], side_m[s, r, 0], 0.0)
    own_units(reduce, outer)

    jumps = (-(bottom.astype(F32)) * SHEAR_JUMP, top.astype(F32) * SHEAR_JUMP)

    def ghost_reduce(d):
        wait_row(1, own_v, row_v, d)
        pl.when(far_side[d] == 0)(lambda: wait_row(2, own_m, row_m, d))
        for j in range(COLS + 2):
            xyzw = row_a[d][window(0, d, j)]
            w = xyzw[3:4]
            far_ratio = w / jnp.where(w > 0.0, far_m[j], 1.0)
            ratio = jnp.where(far_side[d] == 1, far_ratio, row_m[d][j])
            second(3 * d, j, xyzw, row_v[d][window(1, d, j)], ratio, jumps[d])
        for c in range(COLS):
            reduce(d, 2 * d, c)

    near_row(ghost_reduce)
    last_row(ghost_reduce)

    for r in range(ROWS):
        def row_of(k):
            return jnp.concatenate([sums[r, c, k : k + 1, :] for c in range(COLS)], axis=0)

        block = [
            2.0 * pos[r, 0] + (2.0 * column - 8.0),
            2.0 * pos[r, 1] + (2.0 * r - 2.0),
            2.0 * pos[r, 2] - 1.0,
        ]
        inv = inverse_rho[r]
        ratio_sum, mass_sum = row_of(0), row_of(8)
        visc_sum = ratio_sum - SOFT_Q * row_of(16)
        for f in range(3):
            far = block[f] * ratio_sum - row_of(1 + f)
            near_part = block[f] * mass_sum - row_of(9 + f)
            drag = vel[r, f] * visc_sum - (row_of(4 + f) - SOFT_Q * row_of(20 + f))
            total = (-0.5 * SOUND_SQ * GRAD_SCALE) * (inv * near_part + far) + (2.0 * VISCOSITY * GRAD_SCALE) * (inv * drag)
            acc_out[r, f] = jnp.where(valid[r], total, 0.0)

    def drain(copies):
        for copy in copies:
            copy.wait_send()

    drain(sent_a + sent_v + sent_m[2])
    pl.when(top == 1)(lambda: drain(sent_up))
    pl.when(top == 0)(lambda: drain(sent_m[0]))
    pl.when(bottom == 1)(lambda: drain(sent_down))
    pl.when(bottom == 0)(lambda: drain(sent_m[1]))


def put_out(density, accel, density_out, accel_out, sem):
    copies = [
        pltpu.make_async_copy(accel, accel_out, sem.at[0]),
        pltpu.make_async_copy(density, density_out, sem.at[1]),
    ]
    for copy in copies:
        copy.start()
    for copy in copies:
        copy.wait()


def local(ny, nx, position, velocity, particle_mass, cell_counts, shear_shift):
    pos = jnp.transpose(position, (0, 3, 1, 2))
    vel = jnp.transpose(velocity, (0, 3, 1, 2))
    vmem = pl.BlockSpec(memory_space=pltpu.VMEM)
    hbm = pl.BlockSpec(memory_space=pltpu.HBM)
    in_hbm = functools.partial(pltpu.with_memory_space_constraint, memory_space=pltpu.HBM)
    table = (ROWS, 3, COLS, 3 * SLOTS, SLOTS)
    density, accel = pl.pallas_call(
        functools.partial(kernel, ny, nx),
        out_shape=(
            jax.ShapeDtypeStruct((ROWS, COLS, SLOTS), F32),
            jax.ShapeDtypeStruct((ROWS, 3, COLS, SLOTS), F32),
        ),
        in_specs=[hbm, pl.BlockSpec(memory_space=pltpu.SMEM), hbm, hbm, hbm],
        out_specs=(vmem, vmem),
        scratch_shapes=[
            pltpu.VMEM((ROWS, COLS, 4, SLOTS), F32),
            pltpu.VMEM((ROWS, COLS, 4, SLOTS), F32),
            pltpu.VMEM((ROWS, COLS, 1, SLOTS), F32),
            *(pltpu.VMEM((w, f, SLOTS), F32) for _ in range(2) for w, f in zip(WINDOW, (4, 4, 1))),
            *(pltpu.VMEM((2, ROWS, w, f, SLOTS), F32) for w, f in zip(WIDTH, (4, 4, 1))),
            pltpu.VMEM((WINDOW[0], 4, SLOTS), F32),
            pltpu.VMEM((COLS + 2, 1, SLOTS), F32),
            pltpu.VMEM((ROWS + 3, (COLS + 4) * SLOTS, 64), BF16),
            pltpu.VMEM((ROWS, COLS, 64, SLOTS), BF16),
            pltpu.VMEM((COLS + 2, 64, SLOTS), BF16),
            pltpu.VMEM((ROWS + 2, 64, (COLS + 2) * SLOTS), BF16),
            pltpu.VMEM((ROWS + 3, (COLS + 4) * SLOTS, SLOTS), F32),
            pltpu.VMEM(table, BF16),
            pltpu.VMEM(table, BF16),
            pltpu.VMEM(table, BF16),
            pltpu.VMEM((ROWS, COLS, 8, SLOTS), F32),
            pltpu.VMEM((ROWS, COLS, 24, SLOTS), F32),
            pltpu.SMEM((ROWS, COLS), jnp.int32),
            pltpu.VMEM((ROWS, 3, COLS, SLOTS), F32),
            pltpu.VMEM((ROWS, 3, COLS, SLOTS), F32),
            pltpu.VMEM((ROWS, COLS, SLOTS), F32),
            pltpu.SemaphoreType.DMA((4, 8)),
            pltpu.SemaphoreType.DMA((4, 8)),
            pltpu.SemaphoreType.DMA((4,)),
        ],
        compiler_params=pltpu.CompilerParams(
            collective_id=0, has_side_effects=True, vmem_limit_bytes=48 * 1024 * 1024
        ),
        name="sph_step",
    )(in_hbm(cell_counts), shear_shift, in_hbm(pos), in_hbm(vel), in_hbm(particle_mass))
    density, accel = pl.pallas_call(
        put_out,
        out_shape=(
            jax.ShapeDtypeStruct((ROWS, COLS, SLOTS), F32),
            jax.ShapeDtypeStruct((ROWS, 3, COLS, SLOTS), F32),
        ),
        in_specs=[vmem, vmem],
        out_specs=(hbm, hbm),
        scratch_shapes=[pltpu.SemaphoreType.DMA((2,))],
        compiler_params=pltpu.CompilerParams(vmem_limit_bytes=1024 * 1024),
        name="put_out",
    )(density, accel)
    return density, jnp.transpose(accel, (0, 2, 3, 1))


def solution(mesh):
    placed = (
        P("gy", "gx", None, None),
        P("gy", "gx", None, None),
        P("gy", "gx", None),
        P("gy", "gx"),
        P(),
    )
    return jax.shard_map(
        functools.partial(local, mesh.shape["gy"], mesh.shape["gx"]),
        mesh=mesh,
        in_specs=placed,
        out_specs=(P("gy", "gx", None), P("gy", "gx", None, None)),
        check_vma=False,
    )
```

```python
import functools
import math

import jax
import jax.numpy as jnp
from jax import lax
from jax.experimental import pallas as pl
from jax.experimental.pallas import tpu as pltpu
from jax.sharding import PartitionSpec as P

SMOOTHING = 0.5
KERNEL_NORM = 1.0 / (math.pi * SMOOTHING**3)
SOUND_SQ = 0.2
VISCOSITY = 0.05
SOFTENING = 0.0025
SHEAR_JUMP = 1.0

MESH = pl.DeviceIdType.MESH
F32 = jnp.float32
BF16 = jnp.bfloat16
RHO_SCALE = KERNEL_NORM * 0.25
GRAD_SCALE = KERNEL_NORM * 0.75 / (SMOOTHING * SMOOTHING)
SOFT_Q = SOFTENING / (SMOOTHING * SMOOTHING)
TINY_Q = 1e-8
SLOTS = 128
ROWS = 2
COLS = 8
WIDTH = (2, 1, 1)
DRIFT = 4
EDGE = (WIDTH[0] + DRIFT, WIDTH[1] + DRIFT, 1)
WINDOW = tuple(2 * e + COLS for e in EDGE)
FAR = 3
EXTRA = 4


def pieces(p):
    high = p.astype(BF16).astype(F32)
    rest = p - high
    middle = rest.astype(BF16).astype(F32)
    return high, middle, rest - middle


def zeros(n):
    return jnp.zeros((n, SLOTS), F32)


def kernel(
    ny, nx,
    counts_in, shift, pos_in, vel_in, mass_in,
    dens_out, acc_out,
    own_a, own_v, own_m,
    below_a, below_v, below_m,
    above_a, above_v, above_m,
    side_a, side_v, side_m,
    far_a, far_m,
    near, centre, far_centre, feats, mass_cols,
    g_high, g_low, e_part,
    rho_part, sums,
    counts, pos, vel, mass,
    send_sem, recv_sem, load_sem,
):
    gy, gx = lax.axis_index("gy"), lax.axis_index("gx")
    top = gy // (ny - 1)
    bottom = (ny - 1 - gy) // (ny - 1)
    half = nx // 2
    up_y, down_y = lax.rem(gy + 1, ny), lax.rem(gy + ny - 1, ny)

    def up_id(k):
        return (up_y, lax.rem(gx + half * top + k + nx, nx))

    def down_id(k):
        return (down_y, lax.rem(gx + half * bottom + k + nx, nx))

    left_id = (gy, lax.rem(gx + nx - 1, nx))
    right_id = (gy, lax.rem(gx + 1, nx))

    row_a, row_v, row_m = (below_a, above_a), (below_v, above_v), (below_m, above_m)
    barrier = pltpu.get_barrier_semaphore()
    for k in (0, -1, 1):
        pl.semaphore_signal(barrier, inc=1, device_id=up_id(k), device_id_type=MESH)
        pl.semaphore_signal(barrier, inc=1, device_id=down_id(k), device_id_type=MESH)
    pl.semaphore_signal(barrier, inc=1, device_id=left_id, device_id_type=MESH)
    pl.semaphore_signal(barrier, inc=1, device_id=right_id, device_id_type=MESH)

    loads = [
        pltpu.make_async_copy(src, dst, load_sem.at[i])
        for i, (src, dst) in enumerate(
            ((counts_in, counts), (pos_in, pos), (mass_in, mass), (vel_in, vel))
        )
    ]
    for load in loads:
        load.start()

    def copy_of(phase, slot, src, dst, device):
        return pltpu.make_async_remote_copy(
            src_ref=src,
            dst_ref=dst,
            send_sem=send_sem.at[phase, slot],
            recv_sem=recv_sem.at[phase, slot],
            device_id=device,
            device_id_type=MESH,
        )

    def spans(edge):
        return ((0, 0, COLS, edge), (1, COLS - edge, edge, 0), (-1, 0, edge, edge + COLS))

    def row_copies(phase, slot, src, dst, device):
        return [
            copy_of(phase, slot - k, src.at[pl.ds(start, count)], dst.at[pl.ds(at, count)], device(k))
            for k, start, count, at in spans(EDGE[phase % FAR])
        ]

    def up_copies(phase, own, row):
        return row_copies(phase, 1, own.at[1], row[0], up_id)

    def down_copies(phase, own, row):
        return row_copies(phase, 4, own.at[0], row[1], down_id)

    def side_copies(phase, own, side):
        w = WIDTH[phase]
        return [
            copy_of(phase, 6, own.at[:, pl.ds(COLS - w, w)], side.at[0], right_id),
            copy_of(phase, 7, own.at[:, pl.ds(0, w)], side.at[1], left_id),
        ]

    def far_copies():
        return (
            row_copies(FAR, 1, own_a.at[0], far_a, up_id),
            row_copies(FAR, 1, own_a.at[1], far_a, down_id),
        )

    def start(copies):
        for copy in copies:
            copy.start()

    def wait_row(phase, own, row, d, blocks=slice(None)):
        for copy in row_copies(phase, 3 * d + 1, own.at[0], row[d], lambda k: left_id)[blocks]:
            copy.wait_recv()

    def wait_side(phase, own, side):
        for copy in side_copies(phase, own, side):
            copy.wait_recv()

    spot = lax.broadcasted_iota(jnp.int32, (64, SLOTS), 0)
    pick_mass = ((spot == 5) | (spot == 29) | (spot == 45)).astype(F32).astype(BF16)
    lane = lax.broadcasted_iota(jnp.int32, (COLS, SLOTS), 1)
    column = lax.broadcasted_iota(jnp.int32, (COLS, SLOTS), 0).astype(F32)

    def valid_of(r):
        bound = jnp.concatenate([jnp.full((1, SLOTS), counts[r, c], jnp.int32) for c in range(COLS)], axis=0)
        return lane < bound

    for load in loads:
        load.wait()
    for r in range(ROWS):
        fields = [pos[r, 0], pos[r, 1], pos[r, 2], jnp.where(valid_of(r), mass[r], 0.0)]
        for f in range(4):
            for c in range(COLS):
                own_a[r, c, f : f + 1, :] = fields[f][c : c + 1, :]
        for f in range(3):
            for c in range(COLS):
                own_v[r, c, f : f + 1, :] = vel[r, f][c : c + 1, :]
        for c in range(COLS):
            own_v[r, c, 3:4, :] = zeros(1)

    def scaled(xyzw, j, row):
        row = row.astype(F32) if hasattr(row, "astype") else float(row)
        x = 2.0 * xyzw[0:1] + (2.0 * j - 10.0)
        y = 2.0 * xyzw[1:2] + (2.0 * row - 4.0)
        return x, y, 2.0 * xyzw[2:3] - 1.0

    def prepare(e, j, xyzw, row=None):
        x, y, z = scaled(xyzw, j, e if row is None else row)
        w = xyzw[3:4]
        n = x * x + y * y + z * z
        lhs = jnp.concatenate([x, y, z, n, jnp.ones((1, SLOTS), F32), w, zeros(2)], axis=0)
        high, middle, low = pieces(lhs)
        table = jnp.concatenate([high, high, high, middle, middle, low, zeros(16)], axis=0).T
        at = (j + 1) * SLOTS
        near[e, at : at + SLOTS, :] = table.astype(BF16)
        mass_cols[e, at : at + SLOTS, :] = jnp.dot(table.astype(BF16), pick_mass, preferred_element_type=F32)
        if row is None and 0 <= j < COLS + 2:
            first = jnp.concatenate([w, w * x, w * y, w * z, zeros(4)], axis=0)
            feats[e, 32:64, j * SLOTS : (j + 1) * SLOTS] = jnp.concatenate([*pieces(first), zeros(8)], axis=0).astype(BF16)

    def centre_of(xyzw, j, row):
        x, y, z = scaled(xyzw, j, row)
        n = x * x + y * y + z * z
        rhs = jnp.concatenate([-2.0 * x, -2.0 * y, -2.0 * z, jnp.ones((1, SLOTS), F32), n, zeros(3)], axis=0)
        high, middle, low = pieces(rhs)
        return jnp.concatenate([high, middle, low, high, middle, high, zeros(16)], axis=0).astype(BF16)

    def prepare_own(r, carry):
        for c in range(COLS):
            prepare(r + 1, c + 1, own_a[r, c])
            centre[r, c] = centre_of(own_a[r, c], c + 1, r + 1)
        return carry

    sent_a = up_copies(0, own_a, row_a) + down_copies(0, own_a, row_a) + side_copies(0, own_a, side_a)
    sent_v = up_copies(1, own_v, row_v) + down_copies(1, own_v, row_v) + side_copies(1, own_v, side_v)
    sent_up, sent_down = far_copies()

    def exchange():
        pl.semaphore_wait(barrier, 8)
        start(sent_a)
        pl.when(top == 1)(lambda: start(sent_up))
        pl.when(bottom == 1)(lambda: start(sent_down))
        start(sent_v)

    first = (nx - gx) // nx
    patient = jnp.maximum((top + bottom) * (1 - gx // half), first)
    pl.when(patient == 0)(exchange)
    lax.fori_loop(0, ROWS, prepare_own, 0)
    rho_part[...] = jnp.zeros_like(rho_part)
    sums[...] = jnp.zeros_like(sums)

    def kernel_of(cells, rhs):
        q_sq = jnp.maximum(jnp.dot(cells, rhs, preferred_element_type=F32), TINY_Q)
        inverse = lax.rsqrt(q_sq)
        q = q_sq * inverse
        u = jnp.maximum(2.0 - q, 0.0)
        s = jnp.maximum(1.0 - q, 0.0)
        u_sq = u * u
        s_sq = 4.0 * (s * s)
        return u_sq * u - s_sq * s, (s_sq - u_sq) * inverse, q_sq

    def pairs(r, a, c):
        e = r + a
        total = rho_part[r, c]
        rhs = centre[r, c]
        for b in range(3):
            at = (c + b + 1) * SLOTS
            value, slope, q_sq = kernel_of(near[e, at : at + SLOTS, :], rhs)
            soft = lax.rsqrt(q_sq + SOFT_Q)
            extra = (slope * soft) * soft
            weighted = value * mass_cols[e, at : at + SLOTS, :]
            total = total + jnp.sum(weighted.reshape(SLOTS // 8, 8, SLOTS), axis=0)
            high = slope.astype(BF16)
            span = pl.ds(b * SLOTS, SLOTS)
            g_high[r, a, c, span, :] = high
            g_low[r, a, c, span, :] = (slope - high.astype(F32)).astype(BF16)
            e_part[r, a, c, span, :] = extra.astype(BF16)
        rho_part[r, c] = total

    def reduce(r, a, c):
        e = r + a
        lanes = pl.ds(c * SLOTS, 3 * SLOTS)
        rows = feats[e, :, lanes]
        g = jnp.dot(rows, g_high[r, a, c], preferred_element_type=F32)
        g = g + jnp.dot(rows, g_low[r, a, c], preferred_element_type=F32)
        v = jnp.dot(rows[0:32], e_part[r, a, c], preferred_element_type=F32)
        sums[r, c, 0:8, :] += g[0:8] + g[8:16] + g[16:24]
        sums[r, c, 8:16, :] += g[32:40] + g[40:48] + g[48:56]
        sums[r, c, 16:24, :] += v[0:8] + v[8:16] + v[16:24]

    def own_units(work, cells):
        def body(t, carry):
            r = t // 2
            a = 1 - r + lax.rem(t, 2)
            for c in cells:
                work(r, a, c)
            return carry

        lax.fori_loop(0, 4, body, 0)

    inner, outer = tuple(range(1, COLS - 1)), (0, COLS - 1)
    own_units(pairs, inner)
    drift = jnp.clip(shift[0] - half * COLS, -DRIFT, DRIFT)
    drifts = (bottom * drift, -top * drift)
    far_side = (bottom, top)

    def window(phase, d, j):
        return EDGE[phase] - 1 + drifts[d] + j

    def near_row(work):
        pl.when(bottom == 1)(lambda: work(1))
        pl.when(bottom == 0)(lambda: work(0))

    def last_row(work):
        pl.when(bottom == 1)(lambda: work(0))
        pl.when(bottom == 0)(lambda: work(1))

    def ghost_first(d):
        wait_row(0, own_a, row_a, d)
        for j in range(COLS + 2):
            prepare(3 * d, j, row_a[d][window(0, d, j)])
        for c in outer:
            pairs(d, 2 * d, c)

    def ghost_rest(d):
        for c in inner:
            pairs(d, 2 * d, c)

    pl.when(patient == 1)(exchange)

    edge = top + bottom
    near_row(ghost_first)
    pl.when(edge == 1)(lambda: ghost_rest(bottom))
    wait_side(0, own_a, side_a)
    for s in (0, 1):
        for r in range(ROWS):
            prepare(r + 1, (COLS + 1) * s, side_a[s, r, 1 - s])
    own_units(pairs, outer)
    last_row(ghost_first)

    sent_m = up_copies(2, own_m, row_m), down_copies(2, own_m, row_m), side_copies(2, own_m, side_m)
    for r in range(ROWS):
        for c in outer:
            rho = jnp.sum(rho_part[r, c], axis=0, keepdims=True) * RHO_SCALE
            own_m[r, c] = own_a[r, c][3:4] / jnp.where(lane[0:1] < counts[r, c], rho, 1.0)
    start(sent_m[2])
    pl.when(top == 0)(lambda: start(sent_m[0][1:]))
    pl.when(bottom == 0)(lambda: start(sent_m[1][1:]))

    def rest(t, carry):
        ghost_rest(edge * top + (1 - edge) * t)
        return carry

    lax.fori_loop(edge, 2, rest, 0)

    valid = [valid_of(r) for r in range(ROWS)]
    inverse_rho = []
    for r in range(ROWS):
        rho = jnp.concatenate([jnp.sum(rho_part[r, c], axis=0, keepdims=True) for c in range(COLS)], axis=0) * RHO_SCALE
        dens_out[r] = jnp.where(valid[r], rho, 0.0)
        inv = 1.0 / jnp.where(valid[r], rho, 1.0)
        inverse_rho.append(inv)
        ratio = jnp.where(valid[r], mass[r], 0.0) * inv
        for c in inner:
            own_m[r, c] = ratio[c : c + 1, :]
    pl.when(top == 0)(lambda: start(sent_m[0][:1]))
    pl.when(bottom == 0)(lambda: start(sent_m[1][:1]))

    def far_tables(d):
        for copy in row_copies(FAR, 1, own_a.at[0], far_a, lambda k: left_id):
            copy.wait_recv()
        for j in range(-1, COLS + 3):
            prepare(EXTRA, j, far_a[window(0, d, j)], row=5 * d - 1)
        for s in (0, 1):
            j = (COLS + 3) * s - 1
            prepare(3 * d, j, row_a[d][window(0, d, j)])
            prepare(d + 1, j, side_a[s, d, s])
        for j in range(COLS + 2):
            far_centre[j] = centre_of(row_a[d][window(0, d, j)], j, 3 * d)

    def far_density(d):
        def body(t, carry):
            for i in range(5):
                j = 5 * t + i
                total = zeros(8)
                rhs = far_centre[j]
                for n, e in enumerate((d + 1, 3 * d, EXTRA)):
                    for b in range(3):
                        at = pl.multiple_of((j + b) * SLOTS, SLOTS)
                        value, _, _ = kernel_of(near[e, pl.ds(at, SLOTS), :], rhs)
                        weighted = value * mass_cols[e, pl.ds(at, SLOTS), :]
                        total = total + jnp.sum(weighted.reshape(SLOTS // 8, 8, SLOTS), axis=0)
                    turn = 3 * i + n
                    if turn < 2 * len(inner):
                        reduce(t, 1 - t + turn // len(inner), inner[turn % len(inner)])
                far_m[j] = jnp.sum(total, axis=0, keepdims=True) * RHO_SCALE
            return carry

        lax.fori_loop(0, 2, body, 0)

    def second(e, j, xyzw, v, ratio, jump):
        x, y, z = scaled(xyzw, j, e)
        block = jnp.concatenate(
            [ratio, ratio * x, ratio * y, ratio * z, ratio * (v[0:1] + jump), ratio * v[1:2], ratio * v[2:3], zeros(1)],
            axis=0,
        )
        feats[e, 0:32, j * SLOTS : (j + 1) * SLOTS] = jnp.concatenate([*pieces(block), zeros(8)], axis=0).astype(BF16)

    def second_own(r, carry):
        for c in range(COLS):
            second(r + 1, c + 1, own_a[r, c], own_v[r, c], own_m[r, c], 0.0)
        return carry

    lax.fori_loop(0, ROWS, second_own, 0)
    pl.when(bottom == 1)(lambda: far_tables(0))
    pl.when(top == 1)(lambda: far_tables(1))
    pl.when(edge == 1)(lambda: far_density(top))
    pl.when(edge == 0)(lambda: own_units(reduce, inner))
    jumps = (-(bottom.astype(F32)) * SHEAR_JUMP, top.astype(F32) * SHEAR_JUMP)

    def ghost_second(d, blocks, cells):
        pl.when(far_side[d] == 0)(lambda: wait_row(2, own_m, row_m, d, blocks))
        for j in cells:
            xyzw = row_a[d][window(0, d, j)]
            w = xyzw[3:4]
            far_ratio = w / jnp.where(w > 0.0, far_m[j], 1.0)
            ratio = jnp.where(far_side[d] == 1, far_ratio, row_m[d][j])
            second(3 * d, j, xyzw, row_v[d][window(1, d, j)], ratio, jumps[d])

    for d in (0, 1):
        wait_row(1, own_v, row_v, d)
        ghost_second(d, slice(0, 1), range(1, COLS + 1))
        for c in inner:
            reduce(d, 2 * d, c)
    wait_side(1, own_v, side_v)
    wait_side(2, own_m, side_m)
    for s in (0, 1):
        for r in range(ROWS):
            second(r + 1, (COLS + 1) * s, side_a[s, r, 1 - s], side_v[s, r, 0], side_m[s, r, 0], 0.0)
    own_units(reduce, outer)
    for d in (0, 1):
        ghost_second(d, slice(1, 3), (0, COLS + 1))
        for c in outer:
            reduce(d, 2 * d, c)

    for r in range(ROWS):
        def row_of(k):
            return jnp.concatenate([sums[r, c, k : k + 1, :] for c in range(COLS)], axis=0)

        block = [
            2.0 * pos[r, 0] + (2.0 * column - 8.0),
            2.0 * pos[r, 1] + (2.0 * r - 2.0),
            2.0 * pos[r, 2] - 1.0,
        ]
        inv = inverse_rho[r]
        ratio_sum, mass_sum = row_of(0), row_of(8)
        visc_sum = ratio_sum - SOFT_Q * row_of(16)
        for f in range(3):
            far = block[f] * ratio_sum - row_of(1 + f)
            near_part = block[f] * mass_sum - row_of(9 + f)
            drag = vel[r, f] * visc_sum - (row_of(4 + f) - SOFT_Q * row_of(20 + f))
            total = (-0.5 * SOUND_SQ * GRAD_SCALE) * (inv * near_part + far) + (2.0 * VISCOSITY * GRAD_SCALE) * (inv * drag)
            acc_out[r, f] = jnp.where(valid[r], total, 0.0)

    def drain(copies):
        for copy in copies:
            copy.wait_send()

    drain(sent_a + sent_v + sent_m[2])
    pl.when(top == 1)(lambda: drain(sent_up))
    pl.when(top == 0)(lambda: drain(sent_m[0]))
    pl.when(bottom == 1)(lambda: drain(sent_down))
    pl.when(bottom == 0)(lambda: drain(sent_m[1]))


def put_out(density, accel, density_out, accel_out, sem):
    copies = [
        pltpu.make_async_copy(accel, accel_out, sem.at[0]),
        pltpu.make_async_copy(density, density_out, sem.at[1]),
    ]
    for copy in copies:
        copy.start()
    for copy in copies:
        copy.wait()


def local(ny, nx, position, velocity, particle_mass, cell_counts, shear_shift):
    pos = jnp.transpose(position, (0, 3, 1, 2))
    vel = jnp.transpose(velocity, (0, 3, 1, 2))
    vmem = pl.BlockSpec(memory_space=pltpu.VMEM)
    hbm = pl.BlockSpec(memory_space=pltpu.HBM)
    in_hbm = functools.partial(pltpu.with_memory_space_constraint, memory_space=pltpu.HBM)
    table = (ROWS, 3, COLS, 3 * SLOTS, SLOTS)
    density, accel = pl.pallas_call(
        functools.partial(kernel, ny, nx),
        out_shape=(
            jax.ShapeDtypeStruct((ROWS, COLS, SLOTS), F32),
            jax.ShapeDtypeStruct((ROWS, 3, COLS, SLOTS), F32),
        ),
        in_specs=[hbm, pl.BlockSpec(memory_space=pltpu.SMEM), hbm, hbm, hbm],
        out_specs=(vmem, vmem),
        scratch_shapes=[
            pltpu.VMEM((ROWS, COLS, 4, SLOTS), F32),
            pltpu.VMEM((ROWS, COLS, 4, SLOTS), F32),
            pltpu.VMEM((ROWS, COLS, 1, SLOTS), F32),
            *(pltpu.VMEM((w, f, SLOTS), F32) for _ in range(2) for w, f in zip(WINDOW, (4, 4, 1))),
            *(pltpu.VMEM((2, ROWS, w, f, SLOTS), F32) for w, f in zip(WIDTH, (4, 4, 1))),
            pltpu.VMEM((WINDOW[0], 4, SLOTS), F32),
            pltpu.VMEM((COLS + 2, 1, SLOTS), F32),
            pltpu.VMEM((ROWS + 3, (COLS + 4) * SLOTS, 64), BF16),
            pltpu.VMEM((ROWS, COLS, 64, SLOTS), BF16),
            pltpu.VMEM((COLS + 2, 64, SLOTS), BF16),
            pltpu.VMEM((ROWS + 2, 64, (COLS + 2) * SLOTS), BF16),
            pltpu.VMEM((ROWS + 3, (COLS + 4) * SLOTS, SLOTS), F32),
            pltpu.VMEM(table, BF16),
            pltpu.VMEM(table, BF16),
            pltpu.VMEM(table, BF16),
            pltpu.VMEM((ROWS, COLS, 8, SLOTS), F32),
            pltpu.VMEM((ROWS, COLS, 24, SLOTS), F32),
            pltpu.SMEM((ROWS, COLS), jnp.int32),
            pltpu.VMEM((ROWS, 3, COLS, SLOTS), F32),
            pltpu.VMEM((ROWS, 3, COLS, SLOTS), F32),
            pltpu.VMEM((ROWS, COLS, SLOTS), F32),
            pltpu.SemaphoreType.DMA((4, 8)),
            pltpu.SemaphoreType.DMA((4, 8)),
            pltpu.SemaphoreType.DMA((4,)),
        ],
        compiler_params=pltpu.CompilerParams(
            collective_id=0, has_side_effects=True, vmem_limit_bytes=48 * 1024 * 1024
        ),
        name="sph_step",
    )(in_hbm(cell_counts), shear_shift, in_hbm(pos), in_hbm(vel), in_hbm(particle_mass))
    density, accel = pl.pallas_call(
        put_out,
        out_shape=(
            jax.ShapeDtypeStruct((ROWS, COLS, SLOTS), F32),
            jax.ShapeDtypeStruct((ROWS, 3, COLS, SLOTS), F32),
        ),
        in_specs=[vmem, vmem],
        out_specs=(hbm, hbm),
        scratch_shapes=[pltpu.SemaphoreType.DMA((2,))],
        compiler_params=pltpu.CompilerParams(vmem_limit_bytes=1024 * 1024),
        name="put_out",
    )(density, accel)
    return density, jnp.transpose(accel, (0, 2, 3, 1))


def solution(mesh):
    placed = (
        P("gy", "gx", None, None),
        P("gy", "gx", None, None),
        P("gy", "gx", None),
        P("gy", "gx"),
        P(),
    )
    return jax.shard_map(
        functools.partial(local, mesh.shape["gy"], mesh.shape["gx"]),
        mesh=mesh,
        in_specs=placed,
        out_specs=(P("gy", "gx", None), P("gy", "gx", None, None)),
        check_vma=False,
    )
```

```python
import functools
import math

import jax
import jax.numpy as jnp
from jax import lax
from jax.experimental import pallas as pl
from jax.experimental.pallas import tpu as pltpu
from jax.sharding import PartitionSpec as P

SMOOTHING = 0.5
KERNEL_NORM = 1.0 / (math.pi * SMOOTHING**3)
SOUND_SQ = 0.2
VISCOSITY = 0.05
SOFTENING = 0.0025
SHEAR_JUMP = 1.0

MESH = pl.DeviceIdType.MESH
F32 = jnp.float32
BF16 = jnp.bfloat16
RHO_SCALE = KERNEL_NORM * 0.25
GRAD_SCALE = KERNEL_NORM * 0.75 / (SMOOTHING * SMOOTHING)
SOFT_Q = SOFTENING / (SMOOTHING * SMOOTHING)
TINY_Q = 1e-8
SLOTS = 128
ROWS = 2
COLS = 8
WIDTH = (2, 1, 1)
DRIFT = 4
EDGE = (WIDTH[0] + DRIFT, WIDTH[1] + DRIFT, 1)
WINDOW = tuple(2 * e + COLS for e in EDGE)
FAR = 3
EXTRA = 4


def pieces(p):
    high = p.astype(BF16).astype(F32)
    rest = p - high
    middle = rest.astype(BF16).astype(F32)
    return high, middle, rest - middle


def zeros(n):
    return jnp.zeros((n, SLOTS), F32)


def kernel(
    ny, nx,
    counts_in, shift, pos_in, vel_in, mass_in,
    dens_out, acc_out,
    own_a, own_v, own_m,
    below_a, below_v, below_m,
    above_a, above_v, above_m,
    side_a, side_v, side_m,
    far_a, far_m,
    near, centre, far_centre, feats, mass_cols,
    g_high, g_low, e_part,
    rho_part, sums,
    counts, pos, vel, mass,
    send_sem, recv_sem, load_sem,
):
    gy, gx = lax.axis_index("gy"), lax.axis_index("gx")
    top = gy // (ny - 1)
    bottom = (ny - 1 - gy) // (ny - 1)
    half = nx // 2
    up_y, down_y = lax.rem(gy + 1, ny), lax.rem(gy + ny - 1, ny)

    def up_id(k):
        return (up_y, lax.rem(gx + half * top + k + nx, nx))

    def down_id(k):
        return (down_y, lax.rem(gx + half * bottom + k + nx, nx))

    left_id = (gy, lax.rem(gx + nx - 1, nx))
    right_id = (gy, lax.rem(gx + 1, nx))

    row_a, row_v, row_m = (below_a, above_a), (below_v, above_v), (below_m, above_m)
    barrier = pltpu.get_barrier_semaphore()
    for k in (0, -1, 1):
        pl.semaphore_signal(barrier, inc=1, device_id=up_id(k), device_id_type=MESH)
        pl.semaphore_signal(barrier, inc=1, device_id=down_id(k), device_id_type=MESH)
    pl.semaphore_signal(barrier, inc=1, device_id=left_id, device_id_type=MESH)
    pl.semaphore_signal(barrier, inc=1, device_id=right_id, device_id_type=MESH)

    loads = [
        pltpu.make_async_copy(src, dst, load_sem.at[i])
        for i, (src, dst) in enumerate(
            ((counts_in, counts), (pos_in, pos), (mass_in, mass), (vel_in, vel))
        )
    ]
    for load in loads:
        load.start()

    def copy_of(phase, slot, src, dst, device):
        return pltpu.make_async_remote_copy(
            src_ref=src,
            dst_ref=dst,
            send_sem=send_sem.at[phase, slot],
            recv_sem=recv_sem.at[phase, slot],
            device_id=device,
            device_id_type=MESH,
        )

    def spans(edge):
        return ((0, 0, COLS, edge), (1, COLS - edge, edge, 0), (-1, 0, edge, edge + COLS))

    def row_copies(phase, slot, src, dst, device):
        return [
            copy_of(phase, slot - k, src.at[pl.ds(start, count)], dst.at[pl.ds(at, count)], device(k))
            for k, start, count, at in spans(EDGE[phase % FAR])
        ]

    def up_copies(phase, own, row):
        return row_copies(phase, 1, own.at[1], row[0], up_id)

    def down_copies(phase, own, row):
        return row_copies(phase, 4, own.at[0], row[1], down_id)

    def side_copies(phase, own, side):
        w = WIDTH[phase]
        return [
            copy_of(phase, 6, own.at[:, pl.ds(COLS - w, w)], side.at[0], right_id),
            copy_of(phase, 7, own.at[:, pl.ds(0, w)], side.at[1], left_id),
        ]

    def far_copies():
        return (
            row_copies(FAR, 1, own_a.at[0], far_a, up_id),
            row_copies(FAR, 1, own_a.at[1], far_a, down_id),
        )

    def start(copies):
        for copy in copies:
            copy.start()

    def wait_row(phase, own, row, d, blocks=slice(None)):
        for copy in row_copies(phase, 3 * d + 1, own.at[0], row[d], lambda k: left_id)[blocks]:
            copy.wait_recv()

    def wait_side(phase, own, side):
        for copy in side_copies(phase, own, side):
            copy.wait_recv()

    spot = lax.broadcasted_iota(jnp.int32, (64, SLOTS), 0)
    pick_mass = ((spot == 5) | (spot == 29) | (spot == 45)).astype(F32).astype(BF16)
    lane = lax.broadcasted_iota(jnp.int32, (COLS, SLOTS), 1)
    column = lax.broadcasted_iota(jnp.int32, (COLS, SLOTS), 0).astype(F32)

    def valid_of(r):
        bound = jnp.concatenate([jnp.full((1, SLOTS), counts[r, c], jnp.int32) for c in range(COLS)], axis=0)
        return lane < bound

    for load in loads[:3]:
        load.wait()
    for r in range(ROWS):
        fields = [pos[r, 0], pos[r, 1], pos[r, 2], jnp.where(valid_of(r), mass[r], 0.0)]
        for f in range(4):
            for c in range(COLS):
                own_a[r, c, f : f + 1, :] = fields[f][c : c + 1, :]

    def scaled(xyzw, j, row):
        row = row.astype(F32) if hasattr(row, "astype") else float(row)
        x = 2.0 * xyzw[0:1] + (2.0 * j - 10.0)
        y = 2.0 * xyzw[1:2] + (2.0 * row - 4.0)
        return x, y, 2.0 * xyzw[2:3] - 1.0

    def prepare(e, j, xyzw, row=None):
        x, y, z = scaled(xyzw, j, e if row is None else row)
        w = xyzw[3:4]
        n = x * x + y * y + z * z
        lhs = jnp.concatenate([x, y, z, n, jnp.ones((1, SLOTS), F32), w, zeros(2)], axis=0)
        high, middle, low = pieces(lhs)
        table = jnp.concatenate([high, high, high, middle, middle, low, zeros(16)], axis=0).T
        at = (j + 1) * SLOTS
        near[e, at : at + SLOTS, :] = table.astype(BF16)
        mass_cols[e, at : at + SLOTS, :] = jnp.dot(table.astype(BF16), pick_mass, preferred_element_type=F32)
        if row is None and 0 <= j < COLS + 2:
            first = jnp.concatenate([w, w * x, w * y, w * z, zeros(4)], axis=0)
            feats[e, 32:64, j * SLOTS : (j + 1) * SLOTS] = jnp.concatenate([*pieces(first), zeros(8)], axis=0).astype(BF16)

    def centre_of(xyzw, j, row):
        x, y, z = scaled(xyzw, j, row)
        n = x * x + y * y + z * z
        rhs = jnp.concatenate([-2.0 * x, -2.0 * y, -2.0 * z, jnp.ones((1, SLOTS), F32), n, zeros(3)], axis=0)
        high, middle, low = pieces(rhs)
        return jnp.concatenate([high, middle, low, high, middle, high, zeros(16)], axis=0).astype(BF16)

    def prepare_own(r, carry):
        for c in range(COLS):
            prepare(r + 1, c + 1, own_a[r, c])
            centre[r, c] = centre_of(own_a[r, c], c + 1, r + 1)
        return carry

    sent_a = up_copies(0, own_a, row_a) + down_copies(0, own_a, row_a) + side_copies(0, own_a, side_a)
    sent_v = up_copies(1, own_v, row_v) + down_copies(1, own_v, row_v) + side_copies(1, own_v, side_v)
    sent_up, sent_down = far_copies()

    def exchange():
        pl.semaphore_wait(barrier, 8)
        start(sent_a)
        pl.when(top == 1)(lambda: start(sent_up))
        pl.when(bottom == 1)(lambda: start(sent_down))
        loads[3].wait()
        for r in range(ROWS):
            for f in range(3):
                for c in range(COLS):
                    own_v[r, c, f : f + 1, :] = vel[r, f][c : c + 1, :]
            for c in range(COLS):
                own_v[r, c, 3:4, :] = zeros(1)
        start(sent_v)

    first = (nx - gx) // nx
    patient = jnp.maximum((top + bottom) * (1 - gx // half), first)
    pl.when(patient == 0)(exchange)
    lax.fori_loop(0, ROWS, prepare_own, 0)
    rho_part[...] = jnp.zeros_like(rho_part)
    sums[...] = jnp.zeros_like(sums)

    def kernel_of(cells, rhs):
        q_sq = jnp.maximum(jnp.dot(cells, rhs, preferred_element_type=F32), TINY_Q)
        inverse = lax.rsqrt(q_sq)
        q = q_sq * inverse
        u = jnp.maximum(2.0 - q, 0.0)
        s = jnp.maximum(1.0 - q, 0.0)
        u_sq = u * u
        s_sq = 4.0 * (s * s)
        return u_sq * u - s_sq * s, (s_sq - u_sq) * inverse, q_sq

    def pairs(r, a, c):
        e = r + a
        total = rho_part[r, c]
        rhs = centre[r, c]
        for b in range(3):
            at = (c + b + 1) * SLOTS
            value, slope, q_sq = kernel_of(near[e, at : at + SLOTS, :], rhs)
            soft = lax.rsqrt(q_sq + SOFT_Q)
            extra = (slope * soft) * soft
            weighted = value * mass_cols[e, at : at + SLOTS, :]
            total = total + jnp.sum(weighted.reshape(SLOTS // 8, 8, SLOTS), axis=0)
            high = slope.astype(BF16)
            span = pl.ds(b * SLOTS, SLOTS)
            g_high[r, a, c, span, :] = high
            g_low[r, a, c, span, :] = (slope - high.astype(F32)).astype(BF16)
            e_part[r, a, c, span, :] = extra.astype(BF16)
        rho_part[r, c] = total

    def reduce(r, a, c):
        e = r + a
        lanes = pl.ds(c * SLOTS, 3 * SLOTS)
        rows = feats[e, :, lanes]
        g = jnp.dot(rows, g_high[r, a, c], preferred_element_type=F32)
        g = g + jnp.dot(rows, g_low[r, a, c], preferred_element_type=F32)
        v = jnp.dot(rows[0:32], e_part[r, a, c], preferred_element_type=F32)
        sums[r, c, 0:8, :] += g[0:8] + g[8:16] + g[16:24]
        sums[r, c, 8:16, :] += g[32:40] + g[40:48] + g[48:56]
        sums[r, c, 16:24, :] += v[0:8] + v[8:16] + v[16:24]

    def own_units(work, cells):
        def body(t, carry):
            r = t // 2
            a = 1 - r + lax.rem(t, 2)
            for c in cells:
                work(r, a, c)
            return carry

        lax.fori_loop(0, 4, body, 0)

    inner, outer = tuple(range(1, COLS - 1)), (0, COLS - 1)
    own_units(pairs, inner)
    drift = jnp.clip(shift[0] - half * COLS, -DRIFT, DRIFT)
    drifts = (bottom * drift, -top * drift)
    far_side = (bottom, top)

    def window(phase, d, j):
        return EDGE[phase] - 1 + drifts[d] + j

    def near_row(work):
        pl.when(bottom == 1)(lambda: work(1))
        pl.when(bottom == 0)(lambda: work(0))

    def last_row(work):
        pl.when(bottom == 1)(lambda: work(0))
        pl.when(bottom == 0)(lambda: work(1))

    def ghost_first(d):
        wait_row(0, own_a, row_a, d)
        for j in range(COLS + 2):
            prepare(3 * d, j, row_a[d][window(0, d, j)])
        for c in outer:
            pairs(d, 2 * d, c)

    def ghost_rest(d):
        for c in inner:
            pairs(d, 2 * d, c)

    pl.when(patient == 1)(exchange)

    edge = top + bottom
    near_row(ghost_first)
    pl.when(edge == 1)(lambda: ghost_rest(bottom))
    wait_side(0, own_a, side_a)
    for s in (0, 1):
        for r in range(ROWS):
            prepare(r + 1, (COLS + 1) * s, side_a[s, r, 1 - s])
    own_units(pairs, outer)
    last_row(ghost_first)

    sent_m = up_copies(2, own_m, row_m), down_copies(2, own_m, row_m), side_copies(2, own_m, side_m)
    for r in range(ROWS):
        for c in outer:
            rho = jnp.sum(rho_part[r, c], axis=0, keepdims=True) * RHO_SCALE
            own_m[r, c] = own_a[r, c][3:4] / jnp.where(lane[0:1] < counts[r, c], rho, 1.0)
    start(sent_m[2])
    pl.when(top == 0)(lambda: start(sent_m[0][1:]))
    pl.when(bottom == 0)(lambda: start(sent_m[1][1:]))

    def rest(t, carry):
        ghost_rest(edge * top + (1 - edge) * t)
        return carry

    lax.fori_loop(edge, 2, rest, 0)

    valid = [valid_of(r) for r in range(ROWS)]
    inverse_rho = []
    for r in range(ROWS):
        rho = jnp.concatenate([jnp.sum(rho_part[r, c], axis=0, keepdims=True) for c in range(COLS)], axis=0) * RHO_SCALE
        dens_out[r] = jnp.where(valid[r], rho, 0.0)
        inv = 1.0 / jnp.where(valid[r], rho, 1.0)
        inverse_rho.append(inv)
        ratio = jnp.where(valid[r], mass[r], 0.0) * inv
        for c in inner:
            own_m[r, c] = ratio[c : c + 1, :]
    pl.when(top == 0)(lambda: start(sent_m[0][:1]))
    pl.when(bottom == 0)(lambda: start(sent_m[1][:1]))

    def far_tables(d):
        for copy in row_copies(FAR, 1, own_a.at[0], far_a, lambda k: left_id):
            copy.wait_recv()
        for j in range(-1, COLS + 3):
            prepare(EXTRA, j, far_a[window(0, d, j)], row=5 * d - 1)
        for s in (0, 1):
            j = (COLS + 3) * s - 1
            prepare(3 * d, j, row_a[d][window(0, d, j)])
            prepare(d + 1, j, side_a[s, d, s])
        for j in range(COLS + 2):
            far_centre[j] = centre_of(row_a[d][window(0, d, j)], j, 3 * d)

    def far_density(d):
        def body(t, carry):
            for i in range(5):
                j = 5 * t + i
                total = zeros(8)
                rhs = far_centre[j]
                for n, e in enumerate((d + 1, 3 * d, EXTRA)):
                    for b in range(3):
                        at = pl.multiple_of((j + b) * SLOTS, SLOTS)
                        value, _, _ = kernel_of(near[e, pl.ds(at, SLOTS), :], rhs)
                        weighted = value * mass_cols[e, pl.ds(at, SLOTS), :]
                        total = total + jnp.sum(weighted.reshape(SLOTS // 8, 8, SLOTS), axis=0)
                    turn = 3 * i + n
                    if turn < 2 * len(inner):
                        reduce(t, 1 - t + turn // len(inner), inner[turn % len(inner)])
                far_m[j] = jnp.sum(total, axis=0, keepdims=True) * RHO_SCALE
            return carry

        lax.fori_loop(0, 2, body, 0)

    def second(e, j, xyzw, v, ratio, jump):
        x, y, z = scaled(xyzw, j, e)
        block = jnp.concatenate(
            [ratio, ratio * x, ratio * y, ratio * z, ratio * (v[0:1] + jump), ratio * v[1:2], ratio * v[2:3], zeros(1)],
            axis=0,
        )
        feats[e, 0:32, j * SLOTS : (j + 1) * SLOTS] = jnp.concatenate([*pieces(block), zeros(8)], axis=0).astype(BF16)

    def second_own(r, carry):
        for c in range(COLS):
            second(r + 1, c + 1, own_a[r, c], own_v[r, c], own_m[r, c], 0.0)
        return carry

    lax.fori_loop(0, ROWS, second_own, 0)
    pl.when(bottom == 1)(lambda: far_tables(0))
    pl.when(top == 1)(lambda: far_tables(1))
    pl.when(edge == 1)(lambda: far_density(top))
    pl.when(edge == 0)(lambda: own_units(reduce, inner))
    jumps = (-(bottom.astype(F32)) * SHEAR_JUMP, top.astype(F32) * SHEAR_JUMP)

    def ghost_second(d, blocks, cells):
        pl.when(far_side[d] == 0)(lambda: wait_row(2, own_m, row_m, d, blocks))
        for j in cells:
            xyzw = row_a[d][window(0, d, j)]
            w = xyzw[3:4]
            far_ratio = w / jnp.where(w > 0.0, far_m[j], 1.0)
            ratio = jnp.where(far_side[d] == 1, far_ratio, row_m[d][j])
            second(3 * d, j, xyzw, row_v[d][window(1, d, j)], ratio, jumps[d])

    for d in (0, 1):
        wait_row(1, own_v, row_v, d)
        ghost_second(d, slice(0, 1), range(1, COLS + 1))
        for c in inner:
            reduce(d, 2 * d, c)
    wait_side(1, own_v, side_v)
    wait_side(2, own_m, side_m)
    for s in (0, 1):
        for r in range(ROWS):
            second(r + 1, (COLS + 1) * s, side_a[s, r, 1 - s], side_v[s, r, 0], side_m[s, r, 0], 0.0)
    own_units(reduce, outer)
    for d in (0, 1):
        ghost_second(d, slice(1, 3), (0, COLS + 1))
        for c in outer:
            reduce(d, 2 * d, c)

    for r in range(ROWS):
        def row_of(k):
            return jnp.concatenate([sums[r, c, k : k + 1, :] for c in range(COLS)], axis=0)

        block = [
            2.0 * pos[r, 0] + (2.0 * column - 8.0),
            2.0 * pos[r, 1] + (2.0 * r - 2.0),
            2.0 * pos[r, 2] - 1.0,
        ]
        inv = inverse_rho[r]
        ratio_sum, mass_sum = row_of(0), row_of(8)
        visc_sum = ratio_sum - SOFT_Q * row_of(16)
        for f in range(3):
            far = block[f] * ratio_sum - row_of(1 + f)
            near_part = block[f] * mass_sum - row_of(9 + f)
            drag = vel[r, f] * visc_sum - (row_of(4 + f) - SOFT_Q * row_of(20 + f))
            total = (-0.5 * SOUND_SQ * GRAD_SCALE) * (inv * near_part + far) + (2.0 * VISCOSITY * GRAD_SCALE) * (inv * drag)
            acc_out[r, f] = jnp.where(valid[r], total, 0.0)

    def drain(copies):
        for copy in copies:
            copy.wait_send()

    drain(sent_a + sent_v + sent_m[2])
    pl.when(top == 1)(lambda: drain(sent_up))
    pl.when(top == 0)(lambda: drain(sent_m[0]))
    pl.when(bottom == 1)(lambda: drain(sent_down))
    pl.when(bottom == 0)(lambda: drain(sent_m[1]))


def put_out(density, accel, density_out, accel_out, sem):
    copies = [
        pltpu.make_async_copy(accel, accel_out, sem.at[0]),
        pltpu.make_async_copy(density, density_out, sem.at[1]),
    ]
    for copy in copies:
        copy.start()
    for copy in copies:
        copy.wait()


def local(ny, nx, position, velocity, particle_mass, cell_counts, shear_shift):
    pos = jnp.transpose(position, (0, 3, 1, 2))
    vel = jnp.transpose(velocity, (0, 3, 1, 2))
    vmem = pl.BlockSpec(memory_space=pltpu.VMEM)
    hbm = pl.BlockSpec(memory_space=pltpu.HBM)
    in_hbm = functools.partial(pltpu.with_memory_space_constraint, memory_space=pltpu.HBM)
    table = (ROWS, 3, COLS, 3 * SLOTS, SLOTS)
    density, accel = pl.pallas_call(
        functools.partial(kernel, ny, nx),
        out_shape=(
            jax.ShapeDtypeStruct((ROWS, COLS, SLOTS), F32),
            jax.ShapeDtypeStruct((ROWS, 3, COLS, SLOTS), F32),
        ),
        in_specs=[hbm, pl.BlockSpec(memory_space=pltpu.SMEM), hbm, hbm, hbm],
        out_specs=(vmem, vmem),
        scratch_shapes=[
            pltpu.VMEM((ROWS, COLS, 4, SLOTS), F32),
            pltpu.VMEM((ROWS, COLS, 4, SLOTS), F32),
            pltpu.VMEM((ROWS, COLS, 1, SLOTS), F32),
            *(pltpu.VMEM((w, f, SLOTS), F32) for _ in range(2) for w, f in zip(WINDOW, (4, 4, 1))),
            *(pltpu.VMEM((2, ROWS, w, f, SLOTS), F32) for w, f in zip(WIDTH, (4, 4, 1))),
            pltpu.VMEM((WINDOW[0], 4, SLOTS), F32),
            pltpu.VMEM((COLS + 2, 1, SLOTS), F32),
            pltpu.VMEM((ROWS + 3, (COLS + 4) * SLOTS, 64), BF16),
            pltpu.VMEM((ROWS, COLS, 64, SLOTS), BF16),
            pltpu.VMEM((COLS + 2, 64, SLOTS), BF16),
            pltpu.VMEM((ROWS + 2, 64, (COLS + 2) * SLOTS), BF16),
            pltpu.VMEM((ROWS + 3, (COLS + 4) * SLOTS, SLOTS), F32),
            pltpu.VMEM(table, BF16),
            pltpu.VMEM(table, BF16),
            pltpu.VMEM(table, BF16),
            pltpu.VMEM((ROWS, COLS, 8, SLOTS), F32),
            pltpu.VMEM((ROWS, COLS, 24, SLOTS), F32),
            pltpu.SMEM((ROWS, COLS), jnp.int32),
            pltpu.VMEM((ROWS, 3, COLS, SLOTS), F32),
            pltpu.VMEM((ROWS, 3, COLS, SLOTS), F32),
            pltpu.VMEM((ROWS, COLS, SLOTS), F32),
            pltpu.SemaphoreType.DMA((4, 8)),
            pltpu.SemaphoreType.DMA((4, 8)),
            pltpu.SemaphoreType.DMA((4,)),
        ],
        compiler_params=pltpu.CompilerParams(
            collective_id=0, has_side_effects=True, vmem_limit_bytes=48 * 1024 * 1024
        ),
        name="sph_step",
    )(in_hbm(cell_counts), shear_shift, in_hbm(pos), in_hbm(vel), in_hbm(particle_mass))
    density, accel = pl.pallas_call(
        put_out,
        out_shape=(
            jax.ShapeDtypeStruct((ROWS, COLS, SLOTS), F32),
            jax.ShapeDtypeStruct((ROWS, 3, COLS, SLOTS), F32),
        ),
        in_specs=[vmem, vmem],
        out_specs=(hbm, hbm),
        scratch_shapes=[pltpu.SemaphoreType.DMA((2,))],
        compiler_params=pltpu.CompilerParams(vmem_limit_bytes=1024 * 1024),
        name="put_out",
    )(density, accel)
    return density, jnp.transpose(accel, (0, 2, 3, 1))


def solution(mesh):
    placed = (
        P("gy", "gx", None, None),
        P("gy", "gx", None, None),
        P("gy", "gx", None),
        P("gy", "gx"),
        P(),
    )
    return jax.shard_map(
        functools.partial(local, mesh.shape["gy"], mesh.shape["gx"]),
        mesh=mesh,
        in_specs=placed,
        out_specs=(P("gy", "gx", None), P("gy", "gx", None, None)),
        check_vma=False,
    )
```
